256 devices in a mesh: groups: 2 (over z), holders: 128 (over y, x, core).
Axes of the slice: x: 8, y: 8, z: 2, core: 2. Of those that a mesh axis runs over, the one named last changes fastest.
The devices are a block of a 8x8x16 slice.
Arguments:
- q_nope: bfloat16 [2, 256, 128], P(None, ('groups', 'holders')), parts along dimension 1, may hold values from -6 to 6
- q_rope: bfloat16 [2, 256, 64], P(None, ('groups', 'holders')), parts along dimension 1, may hold values from -30 to 30
- w_uk: bfloat16 [2, 16, 128, 512], replicated, may hold values from -0.5 to 0.5
- w_uv: bfloat16 [2, 16, 512, 128], replicated, may hold values from -0.25 to 0.25
- new_latent: bfloat16 [2, 16, 576], P(None, 'groups'), parts along dimension 1, may hold values from -33 to 33
- shallow_cache: bfloat16 [1, 256, 512, 576], P(None, ('groups', 'holders')), parts along dimension 1, may hold values from -30 to 30
- slot_positions: int32 [1, 256, 512], P(None, ('groups', 'holders')), parts along dimension 1, may hold values from 0 to 131071
- slab_map: int32 [1, 256], P(None, 'groups'), parts along dimension 1, may hold values from 0 to 127, each once within a row
- deep_cache: bfloat16 [1, 16, 256, 576], P(None, 'groups'), parts along dimension 1, may hold values from -30 to 30
- deep_positions: int32 [1, 16, 256], P(None, 'groups'), parts along dimension 1, may hold values from 0 to 131071
- lengths: int32 [16], P('groups'), parts along dimension 0, may hold values from 1 to 131072
Outputs:
- attended: bfloat16 [2, 256, 128], P(None, ('groups', 'holders')), parts along dimension 1
The draws below stay inside these ranges and needn't reach their ends.
There are 2 independent parts, one for each index of `groups`. The reference program is written for one: setup_inputs(seed, part) draws one part's arguments, and reference() takes and returns one part's arrays. A program takes and returns all parts, laid end to end along the dimension named above; an argument that names none is the same for every part. Nothing has to cross between parts.
Inputs may be any that keep to these rules, and one draw needn't show every extreme that they name: Each row of slab_map names every slot once; entry b * 16 + s is the slot of request b's slab s.
All inputs are finite; a program needn't handle non-finite values.
Results may differ from the reference program's by a relative error of at most 0.0065.
Values may be sent and summed in bfloat16 or wider, within the bound.
No kernel may reach another device: no remote copies, remote signals or barrier semaphores. Data moves between devices by JAX's collectives and lax.ppermute only.
A program may use at most 64 MiB of HBM per device.

```python
import jax
import jax.numpy as jnp
from jax import lax

HEADS = 16
LATENT = 512
ROPE_DIM = 64
NOPE_DIM = 128
VALUE_DIM = 128
BATCH = 8
SLAB = 512
DEEP_TOK = 256
CONTEXT = 131072
SHALLOW = 1
DEEP = 1
LAYERS = 2
SLABS_REQ = 16
SLOTS = 128
ROWS = 128


def direction_table(key):
    raw = jax.random.normal(jax.random.fold_in(key, 9001), (LAYERS, ROPE_DIM), jnp.float32)
    return 2.0 * jnp.clip(raw, -3.0, 3.0)


def base_values(key, shape):
    return jnp.clip(jax.random.normal(key, shape, jnp.float32), -6.0, 6.0)


def aligned_keys(key, seed_offset, shape, first_layer):
    direction = direction_table(key)[first_layer:first_layer + shape[0]]
    drawn = base_values(jax.random.fold_in(key, seed_offset), shape)
    token_shape = shape[:3] + (1,)
    chosen = jax.random.bernoulli(jax.random.fold_in(key, seed_offset + 1), 0.125, token_shape)
    level = jax.random.uniform(jax.random.fold_in(key, seed_offset + 2), token_shape, jnp.float32, 0.5, 4.0)
    extra = jnp.where(chosen, level, 0.0) * direction[:, None, None, :]
    rotary = drawn[..., LATENT:] + extra
    return jnp.concatenate([drawn[..., :LATENT], rotary], axis=-1).astype(jnp.bfloat16)


def draw_q_rope(key, part):
    direction = direction_table(key)
    drawn = base_values(jax.random.fold_in(key, 11), (LAYERS, ROWS, ROPE_DIM))
    picked = jax.random.uniform(jax.random.fold_in(key, 12), (LAYERS, ROWS, 1), jnp.float32)
    strength = 4.0 * picked
    return (drawn + strength * direction[:, None, :]).astype(jnp.bfloat16)


def draw_new_latent(key, part):
    direction = direction_table(key)
    drawn = base_values(jax.random.fold_in(key, 41), (LAYERS, BATCH, LATENT + ROPE_DIM))
    level = jax.random.uniform(jax.random.fold_in(key, 42), (LAYERS, BATCH, 1), jnp.float32, 0.0, 4.5)
    rotary = drawn[..., LATENT:] + level * direction[:, None, :]
    return jnp.concatenate([drawn[..., :LATENT], rotary], axis=-1).astype(jnp.bfloat16)


def draw_shallow_cache(key, part):
    return aligned_keys(key, 21, (SHALLOW, SLOTS, SLAB, LATENT + ROPE_DIM), 0)


def draw_deep_cache(key, part):
    return aligned_keys(key, 31, (DEEP, BATCH, DEEP_TOK, LATENT + ROPE_DIM), SHALLOW)


def place_ends(drawn, own_key, low, high):
    shape = drawn.shape
    index_at = [jax.random.randint(jax.random.fold_in(own_key, axis), (), 0, shape[axis]) for axis in range(len(shape))]
    drawn = drawn.at[tuple(index_at)].set(low)
    longest = shape.index(max(shape))
    index_at[longest] = (index_at[longest] + 1) % shape[longest]
    return drawn.at[tuple(index_at)].set(high)


def steps_of(own_key, dims, cuts, smallest, top_value):
    def one(dim, blocks):
        heights = jax.random.uniform(jax.random.fold_in(jax.random.fold_in(own_key, 6), dim), (blocks,), jnp.float32, smallest / len(cuts), top_value / len(cuts))
        return jnp.repeat(jnp.exp(heights), dims[dim] // blocks).reshape((-1,) + (1,) * (len(dims) - dim - 1))

    level = one(*cuts[0])
    for cut in cuts[1:]:
        level = level * one(*cut)
    return level


def centred(key, shape, scale, bound, pieces=(), held_as=jnp.bfloat16):
    values = scale * jax.random.normal(key, shape, jnp.float32)
    if pieces:
        values = values * steps_of(key, shape, pieces, -0.22, 0.18)
    return jnp.clip(values, -bound, bound).astype(held_as)


def setup_inputs(seed: int = 0, part: int = 0) -> dict:
    seeds = jax.random.split(jax.random.key(seed), 12)
    part_keys = jax.random.split(jax.random.fold_in(seeds[11], part), 12)
    return {
        "q_nope": centred(part_keys[0], (LAYERS, ROWS, NOPE_DIM), 1.0, 6.0, ((1, 128),)),
        "q_rope": draw_q_rope(jax.random.fold_in(jax.random.fold_in(seeds[11], part), 71), part),
        "w_uk": centred(seeds[2], (LAYERS, HEADS, NOPE_DIM, LATENT), NOPE_DIM ** -0.5, 0.5),
        "w_uv": centred(seeds[3], (LAYERS, HEADS, LATENT, VALUE_DIM), LATENT ** -0.5, 0.25),
        "new_latent": draw_new_latent(jax.random.fold_in(jax.random.fold_in(seeds[11], part), 71), part),
        "shallow_cache": draw_shallow_cache(jax.random.fold_in(jax.random.fold_in(seeds[11], part), 71), part),
        "slot_positions": place_ends(jax.random.randint(part_keys[6], (SHALLOW, SLOTS, SLAB), 0, CONTEXT), jax.random.fold_in(part_keys[6], 1), 0, CONTEXT - 1).astype(jnp.int32),
        "slab_map": jax.vmap(lambda own: jax.random.permutation(own, SLOTS))(jax.random.split(part_keys[7], SHALLOW)).reshape((SHALLOW, SLOTS)).astype(jnp.int32),
        "deep_cache": draw_deep_cache(jax.random.fold_in(jax.random.fold_in(seeds[11], part), 71), part),
        "deep_positions": place_ends(jax.random.randint(part_keys[9], (DEEP, BATCH, DEEP_TOK), 0, CONTEXT), jax.random.fold_in(part_keys[9], 1), 0, CONTEXT - 1).astype(jnp.int32),
        "lengths": place_ends(jax.random.randint(part_keys[10], (BATCH,), 1, CONTEXT + 1), jax.random.fold_in(part_keys[10], 1), 1, CONTEXT).astype(jnp.int32),
    }


score_scale = 192.0 ** -0.5
neg_fill = -1.0e30


def one_request(items):
    query, keys, positions, length, newlat = items
    qf = query.astype(jnp.float32)
    kf = keys.astype(jnp.float32)
    score = jnp.einsum('hc,ksc->hks', qf, kf, precision=lax.Precision.HIGHEST) * score_scale
    live = (positions < length)[None]
    block_max = jnp.max(jnp.where(live, score, neg_fill), axis=-1)
    weight = jnp.where(live, jnp.exp(jnp.where(live, score - block_max[..., None], 0.0)), 0.0).astype(jnp.bfloat16)
    wf = weight.astype(jnp.float32)
    block_sum = jnp.sum(wf, axis=-1)
    block_out = jnp.einsum('hks,ksc->hkc', wf, kf[..., :LATENT], precision=lax.Precision.HIGHEST)
    newf = newlat.astype(jnp.float32)
    own_score = jnp.sum(qf * newf[None, :], axis=-1) * score_scale
    top = jnp.maximum(own_score, jnp.max(block_max, axis=-1))
    factor = jnp.exp(block_max - top[:, None])
    own_factor = jnp.exp(own_score - top)
    total = own_factor + jnp.sum(block_sum * factor, axis=-1)
    mixed = own_factor[:, None] * newf[None, :LATENT] + jnp.einsum('hk,hkc->hc', factor, block_out, precision=lax.Precision.HIGHEST)
    return (mixed / total[:, None]).astype(jnp.bfloat16)


def reference(q_nope, q_rope, w_uk, w_uv, new_latent, shallow_cache, slot_positions, slab_map, deep_cache, deep_positions, lengths):
    results = []
    for layer in range(LAYERS):
        nope = q_nope[layer].reshape(BATCH, HEADS, NOPE_DIM).astype(jnp.float32)
        q_lat = jnp.einsum('bhd,hdc->bhc', nope, w_uk[layer].astype(jnp.float32), precision=lax.Precision.HIGHEST).astype(jnp.bfloat16)
        query = jnp.concatenate([q_lat, q_rope[layer].reshape(BATCH, HEADS, ROPE_DIM)], axis=-1)
        if layer < SHALLOW:
            order = slab_map[layer]
            keys = shallow_cache[layer][order].reshape(BATCH, SLABS_REQ, SLAB, LATENT + ROPE_DIM)
            positions = slot_positions[layer][order].reshape(BATCH, SLABS_REQ, SLAB)
        else:
            keys = deep_cache[layer - SHALLOW][:, None]
            positions = deep_positions[layer - SHALLOW][:, None]
        mixed = lax.map(one_request, (query, keys, positions, lengths, new_latent[layer]))
        attended = jnp.einsum('bhc,hcv->bhv', mixed.astype(jnp.float32), w_uv[layer].astype(jnp.float32), precision=lax.Precision.HIGHEST)
        results.append(attended.astype(jnp.bfloat16).reshape(ROWS, VALUE_DIM))
    return jnp.stack(results, axis=0)
```

```python
import jax
import jax.numpy as jnp
from jax import lax
from jax.experimental import pallas as pl
from jax.experimental.pallas import tpu as pltpu
from jax.sharding import PartitionSpec as P

HEADS = 16
LATENT = 512
SLABS_REQ = 16
LANES = 128
CHUNKS = LATENT // LANES
MSG = 8

score_scale = 192.0 ** (-0.5)
neg_fill = -1e30
f32 = jnp.float32
bf16 = jnp.bfloat16


def iota(shape, dim):
    return lax.broadcasted_iota(jnp.int32, shape, dim)


def nt_dot(a, b):
    return lax.dot_general(a, b, (((1,), (1,)), ((), ())), preferred_element_type=f32)


def nn_dot(a, b):
    return jnp.dot(a, b, preferred_element_type=f32)


def picked_row(rows, at):
    rows = rows.astype(f32)
    return jnp.sum(jnp.where(iota(rows.shape, 0) == at, rows, 0.0), axis=0, keepdims=True)


def prep_kernel(nope_ref, rope_ref, out_ref):
    nope = nope_ref[0, :1].astype(f32)
    rope = rope_ref[0, :1].astype(f32)
    rope = jnp.concatenate([rope, jnp.zeros((1, LANES - rope.shape[1]), f32)], axis=1)
    shape = (out_ref.shape[0], LANES)
    pair = jnp.where(iota(shape, 0) % 2 == 0, nope, rope)
    out_ref[...] = pair.astype(bf16)


def attend_kernel(
    idx_ref,
    lengths_ref,
    got_ref,
    nope_ref,
    rope_ref,
    w_uk_ref,
    w_uv_ref,
    newlat_ref,
    slab_ref,
    slab_pos_ref,
    map_ref,
    deep_ref,
    deep_pos_ref,
    send_ref,
    aux_ref,
):
    holder = idx_ref[0]
    own_req = holder // HEADS
    own_head = holder % HEADS

    owners = map_ref[...]
    place = iota(owners.shape, 1) // SLABS_REQ
    req_v = jnp.sum(jnp.where(owners == holder, place, 0), axis=1, keepdims=True)
    req = jnp.sum(req_v)

    rows = got_ref.shape[0]
    part = iota((2 * HEADS, rows), 0)
    want = (req_v * HEADS + part % HEADS) * 2 + part // HEADS
    pick = jnp.where(iota((2 * HEADS, rows), 1) == want, 1.0, 0.0).astype(bf16)
    q_all = nn_dot(pick, got_ref[...]).astype(bf16)
    rope_dim = rope_ref.shape[-1]
    q_nope, q_rope = q_all[:HEADS], q_all[HEADS:, :rope_dim]

    wide = jnp.concatenate([q_nope] * HEADS, axis=1)
    diagonal = iota(wide.shape, 1) // q_nope.shape[1] == iota(wide.shape, 0)
    wide = jnp.where(diagonal, wide, jnp.zeros_like(wide))
    w_uk = w_uk_ref[0].reshape(wide.shape[1], LATENT)
    q_lat = nn_dot(wide, w_uk).astype(bf16)

    latent = slab_ref[0, 0, :LATENT]
    rotary = slab_ref[0, 0, LATENT:]
    score = (nn_dot(q_lat, latent) + nn_dot(q_rope, rotary)) * score_scale
    live = slab_pos_ref[0] < lengths_ref[req]
    top = jnp.max(jnp.where(live, score, neg_fill), axis=1, keepdims=True)
    weight = jnp.where(live, jnp.exp(jnp.where(live, score - top, 0.0)), 0.0).astype(bf16)
    total = jnp.sum(weight.astype(f32), axis=1, keepdims=True)
    safe = jnp.where(total > 0.0, total, 1.0)
    out = nt_dot(weight, latent) / safe
    level = jnp.where(total > 0.0, top + jnp.log(safe), neg_fill)

    blocks = [out[:, j * LANES : (j + 1) * LANES].astype(bf16) for j in range(CHUNKS)]
    rest = jnp.broadcast_to(level, (HEADS, LANES))
    for _ in range(3):
        piece = rest.astype(bf16)
        blocks.append(piece)
        rest = rest - piece.astype(f32)
    stacked = jnp.concatenate(blocks, axis=0)
    shape = (HEADS * MSG, stacked.shape[0])
    line, column = iota(shape, 0), iota(shape, 1)
    place = (line % MSG) * HEADS + line // MSG
    spread = jnp.where((column == place) & (line % MSG < len(blocks)), 1.0, 0.0).astype(bf16)
    message = nn_dot(spread, stacked).astype(bf16)
    send_ref[pl.ds(pl.multiple_of(req * (HEADS * MSG), HEADS * MSG), HEADS * MSG), :] = message

    nope, rope = nope_ref[0], rope_ref[0]
    own_lat = nn_dot(nope[:1], w_uk_ref[0, own_head]).astype(bf16).astype(f32)
    newlat = picked_row(newlat_ref[0], own_req)
    own_score = (
        jnp.sum(own_lat * newlat[:, :LATENT], axis=1, keepdims=True)
        + jnp.sum(rope[:1].astype(f32) * newlat[:, LATENT:], axis=1, keepdims=True)
    ) * score_scale
    for j in range(CHUNKS):
        aux_ref[j : j + 1, :] = newlat[:, j * LANES : (j + 1) * LANES]
    aux_ref[CHUNKS : CHUNKS + 1, :] = jnp.broadcast_to(own_score, (1, LANES))

    own_lat = nn_dot(nope[1:], w_uk_ref[1, own_head]).astype(bf16)
    latent = deep_ref[0, own_req, :LATENT]
    rotary = deep_ref[0, own_req, LATENT:]
    score = (nn_dot(own_lat, latent) + nn_dot(rope[1:], rotary)) * score_scale
    live = deep_pos_ref[0, pl.ds(own_req, 1), :] < lengths_ref[own_req]
    block_max = jnp.max(jnp.where(live, score, neg_fill), axis=1, keepdims=True)
    weight = jnp.where(live, jnp.exp(jnp.where(live, score - block_max, 0.0)), 0.0).astype(bf16)
    block_sum = jnp.sum(weight.astype(f32), axis=1, keepdims=True)
    block_out = nt_dot(weight, latent)
    newlat = picked_row(newlat_ref[1], own_req)
    own_score = (
        jnp.sum(own_lat.astype(f32) * newlat[:, :LATENT], axis=1, keepdims=True)
        + jnp.sum(rope[1:].astype(f32) * newlat[:, LATENT:], axis=1, keepdims=True)
    ) * score_scale
    top = jnp.maximum(own_score, block_max)
    own_factor = jnp.exp(own_score - top)
    far_factor = jnp.exp(block_max - top)
    total = own_factor + block_sum * far_factor
    mixed = ((own_factor * newlat[:, :LATENT] + block_out * far_factor) / total).astype(bf16)
    aux_ref[CHUNKS + 1 : CHUNKS + 2, :] = nn_dot(mixed, w_uv_ref[1, own_head])
    aux_ref[CHUNKS + 2 :, :] = jnp.zeros((MSG - CHUNKS - 2, LANES), f32)


def combine_kernel(idx_ref, map_ref, got_ref, aux_ref, w_uv_ref, out_ref):
    holder = idx_ref[0]
    own_req = holder // HEADS
    own_head = holder % HEADS
    own = aux_ref[...]
    own_score = own[CHUNKS : CHUNKS + 1]
    messages, levels = [], []
    top = own_score
    for s in range(SLABS_REQ):
        slot = map_ref[0, own_req * SLABS_REQ + s]
        message = got_ref[pl.ds(pl.multiple_of(slot * MSG, MSG), MSG), :].astype(f32)
        level = message[CHUNKS : CHUNKS + 1] + (
            message[CHUNKS + 1 : CHUNKS + 2] + message[CHUNKS + 2 : CHUNKS + 3]
        )
        messages.append(message)
        levels.append(level)
        top = jnp.maximum(top, level)
    total = jnp.exp(own_score - top)
    mixed = total * own
    for message, level in zip(messages, levels):
        factor = jnp.exp(level - top)
        total = total + factor
        mixed = mixed + factor * message
    mixed = (mixed / total).astype(bf16).astype(f32)
    row = jnp.concatenate([mixed[j : j + 1] for j in range(CHUNKS)], axis=1).astype(bf16)
    out = jnp.concatenate([nn_dot(row, w_uv_ref[0, own_head]), own[CHUNKS + 1 : CHUNKS + 2]], axis=0)
    out_ref[0] = out.astype(bf16)


VMEM = pl.BlockSpec(memory_space=pltpu.VMEM)
SMEM = pl.BlockSpec(memory_space=pltpu.SMEM)


def call(kernel, out_shape, in_specs, flops):
    many = isinstance(out_shape, tuple)
    return pl.pallas_call(
        kernel,
        out_shape=out_shape,
        in_specs=in_specs,
        out_specs=(VMEM,) * len(out_shape) if many else VMEM,
        compiler_params=pltpu.CompilerParams(vmem_limit_bytes=12 * 1024 * 1024),
        cost_estimate=pl.CostEstimate(flops=flops, bytes_accessed=1 << 20, transcendentals=0),
    )


def exchanged(rows, per_device):
    holders = lax.axis_size("holders")
    tiles = rows.reshape(holders, per_device, LANES)
    return lax.all_to_all(tiles, "holders", 0, 0, tiled=True).reshape(rows.shape)


def shards(
    q_nope,
    q_rope,
    w_uk,
    w_uv,
    new_latent,
    shallow_cache,
    slot_positions,
    slab_map,
    deep_cache,
    deep_positions,
    lengths,
):
    holders = lax.axis_size("holders")
    holder = lax.axis_index("holders").astype(jnp.int32).reshape(1)
    shape = jax.ShapeDtypeStruct
    q_nope, q_rope = q_nope.swapaxes(0, 1), q_rope.swapaxes(0, 1)
    shallow_cache, deep_cache = shallow_cache.swapaxes(2, 3), deep_cache.swapaxes(2, 3)
    queries = call(prep_kernel, shape((holders * 2, LANES), bf16), [VMEM] * 2, 1 << 33)(
        q_nope, q_rope
    )
    queries, holder = lax.optimization_barrier((queries, holder))
    queries = exchanged(queries, 2)
    partials, aux = call(
        attend_kernel,
        (shape((holders * MSG, LANES), bf16), shape((MSG, LANES), f32)),
        [SMEM, SMEM] + [VMEM] * 11,
        1 << 24,
    )(
        holder,
        lengths,
        queries,
        q_nope,
        q_rope,
        w_uk,
        w_uv,
        new_latent,
        shallow_cache,
        slot_positions,
        slab_map,
        deep_cache,
        deep_positions,
    )
    partials = exchanged(partials, MSG)
    rows = call(combine_kernel, shape(q_nope.shape, bf16), [SMEM, SMEM] + [VMEM] * 3, 1 << 20)(
        holder, slab_map, partials, aux, w_uv
    )
    return rows.swapaxes(0, 1)


def solution(mesh):
    spread = ("groups", "holders")
    in_specs = (
        P(None, spread, None),
        P(None, spread, None),
        P(),
        P(),
        P(None, "groups", None),
        P(None, spread, None, None),
        P(None, spread, None),
        P(None, "groups"),
        P(None, "groups", None, None),
        P(None, "groups", None),
        P("groups"),
    )
    return jax.shard_map(
        shards, mesh=mesh, in_specs=in_specs, out_specs=P(None, spread, None), check_vma=False
    )
```

```python
import jax
import jax.numpy as jnp
from jax import lax
from jax.experimental import pallas as pl
from jax.experimental.pallas import tpu as pltpu
from jax.sharding import Mesh
from jax.sharding import PartitionSpec as P

HEADS = 16
LATENT = 512
NOPE = 128
SLABS_REQ = 16
LANES = 128
CHUNKS = LATENT // LANES
MSG = 8
CORES = 2

score_scale = 192.0 ** (-0.5)
neg_fill = -1e30
f32 = jnp.float32
bf16 = jnp.bfloat16


def iota(shape, dim):
    return lax.broadcasted_iota(jnp.int32, shape, dim)


def nt_dot(a, b):
    return lax.dot_general(a, b, (((1,), (1,)), ((), ())), preferred_element_type=f32)


def nn_dot(a, b):
    return jnp.dot(a, b, preferred_element_type=f32)


def picked_row(rows, at):
    rows = rows.astype(f32)
    return jnp.sum(jnp.where(iota(rows.shape, 0) == at, rows, 0.0), axis=0, keepdims=True)


def prep_kernel(idx_ref, query_ref, far_nope_ref, far_rope_ref, out_ref):
    first = idx_ref[0] % CORES == 0

    def padded(row):
        row = row.astype(f32)
        return jnp.concatenate([row, jnp.zeros((1, LANES - row.shape[1]), f32)], axis=1)

    own = query_ref[0, :1, :NOPE].astype(f32), padded(query_ref[0, :1, NOPE:])
    far = far_nope_ref[0, :1].astype(f32), padded(far_rope_ref[0, :1])
    shape = (out_ref.shape[0], LANES)
    line = iota(shape, 0) % (2 * CORES)
    near = (line < 2) == first
    rows = jnp.where(
        near, jnp.where(line % 2 == 0, own[0], own[1]), jnp.where(line % 2 == 0, far[0], far[1])
    )
    out_ref[...] = rows.astype(bf16)


def attend_kernel(
    idx_ref,
    lengths_ref,
    got_ref,
    query_ref,
    w_uk_ref,
    w_uv_ref,
    newlat_ref,
    slab_ref,
    slab_pos_ref,
    map_ref,
    deep_ref,
    deep_pos_ref,
    send_ref,
    aux_ref,
):
    holder = idx_ref[0]
    own_req = holder // HEADS
    own_head = holder % HEADS

    owners = map_ref[...]
    place = iota(owners.shape, 1) // SLABS_REQ
    req_v = jnp.sum(jnp.where(owners == holder, place, 0), axis=1, keepdims=True)
    req = jnp.sum(req_v)

    rows = got_ref.shape[0]
    part = iota((2 * HEADS, rows), 0)
    want = (req_v * HEADS + part % HEADS) * 2 + part // HEADS
    pick = jnp.where(iota((2 * HEADS, rows), 1) == want, 1.0, 0.0).astype(bf16)
    q_all = nn_dot(pick, got_ref[...]).astype(bf16)
    rope_dim = query_ref.shape[-1] - NOPE
    q_nope, q_rope = q_all[:HEADS], q_all[HEADS:, :rope_dim]

    wide = jnp.concatenate([q_nope] * HEADS, axis=1)
    diagonal = iota(wide.shape, 1) // q_nope.shape[1] == iota(wide.shape, 0)
    wide = jnp.where(diagonal, wide, jnp.zeros_like(wide))
    w_uk = w_uk_ref[0].reshape(wide.shape[1], LATENT)
    q_lat = nn_dot(wide, w_uk).astype(bf16)

    latent = slab_ref[0, 0, :LATENT]
    rotary = slab_ref[0, 0, LATENT:]
    score = (nn_dot(q_lat, latent) + nn_dot(q_rope, rotary)) * score_scale
    live = slab_pos_ref[0] < lengths_ref[req]
    top = jnp.max(jnp.where(live, score, neg_fill), axis=1, keepdims=True)
    weight = jnp.where(live, jnp.exp(jnp.where(live, score - top, 0.0)), 0.0).astype(bf16)
    total = jnp.sum(weight.astype(f32), axis=1, keepdims=True)
    safe = jnp.where(total > 0.0, total, 1.0)
    out = nt_dot(weight, latent) / safe
    level = jnp.where(total > 0.0, top + jnp.log(safe), neg_fill)

    blocks = [out[:, j * LANES : (j + 1) * LANES].astype(bf16) for j in range(CHUNKS)]
    rest = jnp.broadcast_to(level, (HEADS, LANES))
    for _ in range(3):
        piece = rest.astype(bf16)
        blocks.append(piece)
        rest = rest - piece.astype(f32)
    stacked = jnp.concatenate(blocks, axis=0)
    shape = (HEADS * MSG, stacked.shape[0])
    line, column = iota(shape, 0), iota(shape, 1)
    place = (line % MSG) * HEADS + line // MSG
    spread = jnp.where((column == place) & (line % MSG < len(blocks)), 1.0, 0.0).astype(bf16)
    message = nn_dot(spread, stacked).astype(bf16)
    send_ref[pl.ds(pl.multiple_of(req * (HEADS * MSG), HEADS * MSG), HEADS * MSG), :] = message

    nope, rope = query_ref[0, :, :NOPE], query_ref[0, :, NOPE:]
    own_lat = nn_dot(nope[:1], w_uk_ref[0, own_head]).astype(bf16).astype(f32)
    newlat = picked_row(newlat_ref[0], own_req)
    own_score = (
        jnp.sum(own_lat * newlat[:, :LATENT], axis=1, keepdims=True)
        + jnp.sum(rope[:1].astype(f32) * newlat[:, LATENT:], axis=1, keepdims=True)
    ) * score_scale
    for j in range(CHUNKS):
        aux_ref[j : j + 1, :] = newlat[:, j * LANES : (j + 1) * LANES]
    aux_ref[CHUNKS : CHUNKS + 1, :] = jnp.broadcast_to(own_score, (1, LANES))

    own_lat = nn_dot(nope[1:], w_uk_ref[1, own_head]).astype(bf16)
    latent = deep_ref[0, own_req, :LATENT]
    rotary = deep_ref[0, own_req, LATENT:]
    score = (nn_dot(own_lat, latent) + nn_dot(rope[1:], rotary)) * score_scale
    live = deep_pos_ref[0, pl.ds(own_req, 1), :] < lengths_ref[own_req]
    block_max = jnp.max(jnp.where(live, score, neg_fill), axis=1, keepdims=True)
    weight = jnp.where(live, jnp.exp(jnp.where(live, score - block_max, 0.0)), 0.0).astype(bf16)
    block_sum = jnp.sum(weight.astype(f32), axis=1, keepdims=True)
    block_out = nt_dot(weight, latent)
    newlat = picked_row(newlat_ref[1], own_req)
    own_score = (
        jnp.sum(own_lat.astype(f32) * newlat[:, :LATENT], axis=1, keepdims=True)
        + jnp.sum(rope[1:].astype(f32) * newlat[:, LATENT:], axis=1, keepdims=True)
    ) * score_scale
    top = jnp.maximum(own_score, block_max)
    own_factor = jnp.exp(own_score - top)
    far_factor = jnp.exp(block_max - top)
    total = own_factor + block_sum * far_factor
    mixed = ((own_factor * newlat[:, :LATENT] + block_out * far_factor) / total).astype(bf16)
    aux_ref[CHUNKS + 1 : CHUNKS + 2, :] = nn_dot(mixed, w_uv_ref[1, own_head])
    aux_ref[CHUNKS + 2 :, :] = jnp.zeros((MSG - CHUNKS - 2, LANES), f32)


def combine_kernel(idx_ref, map_ref, got_ref, far_ref, aux_ref, w_uv_ref, out_ref):
    holder = idx_ref[0]
    own_req = holder // HEADS
    own_head = holder % HEADS
    core = holder % CORES
    own = aux_ref[...]
    own_score = own[CHUNKS : CHUNKS + 1]
    messages, levels = [], []
    top = own_score
    for s in range(SLABS_REQ):
        slot = map_ref[0, own_req * SLABS_REQ + s]
        at = pl.ds(pl.multiple_of(((slot // CORES) * CORES + core) * MSG, MSG), MSG)
        message = jnp.where(slot % CORES == core, got_ref[at, :], far_ref[at, :]).astype(f32)
        level = message[CHUNKS : CHUNKS + 1] + (
            message[CHUNKS + 1 : CHUNKS + 2] + message[CHUNKS + 2 : CHUNKS + 3]
        )
        messages.append(message)
        levels.append(level)
        top = jnp.maximum(top, level)
    total = jnp.exp(own_score - top)
    mixed = total * own
    for message, level in zip(messages, levels):
        factor = jnp.exp(level - top)
        total = total + factor
        mixed = mixed + factor * message
    mixed = (mixed / total).astype(bf16).astype(f32)
    row = jnp.concatenate([mixed[j : j + 1] for j in range(CHUNKS)], axis=1).astype(bf16)
    out = jnp.concatenate([nn_dot(row, w_uv_ref[0, own_head]), own[CHUNKS + 1 : CHUNKS + 2]], axis=0)
    out_ref[0] = out.astype(bf16)


VMEM = pl.BlockSpec(memory_space=pltpu.VMEM)
SMEM = pl.BlockSpec(memory_space=pltpu.SMEM)


def call(kernel, out_shape, in_specs, flops):
    many = isinstance(out_shape, tuple)
    return pl.pallas_call(
        kernel,
        out_shape=out_shape,
        in_specs=in_specs,
        out_specs=(VMEM,) * len(out_shape) if many else VMEM,
        compiler_params=pltpu.CompilerParams(vmem_limit_bytes=12 << 20),
        cost_estimate=pl.CostEstimate(flops=flops, bytes_accessed=1 << 20, transcendentals=0),
    )


def exchanged(rows, per_chip):
    chips = lax.axis_size("chips")
    tiles = rows.reshape(chips, per_chip, LANES)
    return lax.all_to_all(tiles, "chips", 0, 0, tiled=True).reshape(rows.shape)


def swapped(x):
    return lax.ppermute(x, "cores", [(k, (k + 1) % CORES) for k in range(CORES)])


def shards(
    q_nope,
    q_rope,
    w_uk,
    w_uv,
    new_latent,
    shallow_cache,
    slot_positions,
    slab_map,
    deep_cache,
    deep_positions,
    lengths,
):
    chips = lax.axis_size("chips")
    holder = lax.axis_index("chips") * CORES + lax.axis_index("cores")
    holder = holder.astype(jnp.int32).reshape(1)
    shape = jax.ShapeDtypeStruct
    q_nope, q_rope = q_nope.swapaxes(0, 1), q_rope.swapaxes(0, 1)
    shallow_cache, deep_cache = shallow_cache.swapaxes(2, 3), deep_cache.swapaxes(2, 3)
    far_nope, far_rope = swapped(q_nope), swapped(q_rope)
    query = jnp.concatenate([q_nope, q_rope], axis=-1)
    queries = call(
        prep_kernel, shape((chips * CORES * 2, LANES), bf16), [SMEM] + [VMEM] * 3, 1 << 33
    )(holder, query, far_nope, far_rope)
    queries = exchanged(queries, CORES * 2)
    partials, aux = call(
        attend_kernel,
        (shape((chips * CORES * MSG, LANES), bf16), shape((MSG, LANES), f32)),
        [SMEM, SMEM] + [VMEM] * 10,
        1 << 24,
    )(
        holder,
        lengths,
        queries,
        query,
        w_uk,
        w_uv,
        new_latent,
        shallow_cache,
        slot_positions,
        slab_map,
        deep_cache,
        deep_positions,
    )
    partials = exchanged(partials, CORES * MSG)
    rows = call(combine_kernel, shape(q_nope.shape, bf16), [SMEM, SMEM] + [VMEM] * 4, 1 << 20)(
        holder, slab_map, partials, swapped(partials), aux, w_uv
    )
    return rows.swapaxes(0, 1)


def solution(mesh):
    groups, holders = mesh.shape["groups"], mesh.shape["holders"]
    mesh = Mesh(
        mesh.devices.reshape(groups, holders // CORES, CORES), ("groups", "chips", "cores")
    )
    spread = ("groups", "chips", "cores")
    in_specs = (
        P(None, spread, None),
        P(None, spread, None),
        P(),
        P(),
        P(None, "groups", None),
        P(None, spread, None, None),
        P(None, spread, None),
        P(None, "groups"),
        P(None, "groups", None, None),
        P(None, "groups", None),
        P("groups"),
    )
    return jax.shard_map(
        shards, mesh=mesh, in_specs=in_specs, out_specs=P(None, spread, None), check_vma=False
    )
```

```python
import math

import jax
import jax.numpy as jnp
from jax import lax
from jax.experimental import pallas as pl
from jax.experimental.pallas import tpu as pltpu
from jax.sharding import Mesh
from jax.sharding import PartitionSpec as P

HEADS = 16
LATENT = 512
NOPE = 128
SLABS_REQ = 16
LANES = 128
CHUNKS = LATENT // LANES
MSG = 8
CORES = 2
LOG_2 = math.log(2.0)

score_scale = 192.0 ** (-0.5)
neg_fill = -1e30
f32 = jnp.float32
bf16 = jnp.bfloat16


def iota(shape, dim):
    return lax.broadcasted_iota(jnp.int32, shape, dim)


def nt_dot(a, b):
    return lax.dot_general(a, b, (((1,), (1,)), ((), ())), preferred_element_type=f32)


def nn_dot(a, b):
    return jnp.dot(a, b, preferred_element_type=f32)


def picked_row(rows, at):
    rows = rows.astype(f32)
    return jnp.sum(jnp.where(iota(rows.shape, 0) == at, rows, 0.0), axis=0, keepdims=True)


def pieces(x):
    out = []
    for _ in range(3):
        out.append(x.astype(bf16))
        x = x - out[-1].astype(f32)
    return out


def message_level(message):
    rows = [message[..., CHUNKS + j : CHUNKS + j + 1, :] for j in range(3)]
    return rows[0] + (rows[1] + rows[2])


def prep_kernel(idx_ref, query_ref, far_nope_ref, far_rope_ref, out_ref):
    first = idx_ref[0] % CORES == 0

    def padded(row):
        row = row.astype(f32)
        return jnp.concatenate([row, jnp.zeros((1, LANES - row.shape[1]), f32)], axis=1)

    own = query_ref[0, :1, :NOPE].astype(f32), padded(query_ref[0, :1, NOPE:])
    far = far_nope_ref[0, :1].astype(f32), padded(far_rope_ref[0, :1])
    shape = (out_ref.shape[0], LANES)
    line = iota(shape, 0) % (2 * CORES)
    near = (line < 2) == first
    rows = jnp.where(
        near, jnp.where(line % 2 == 0, own[0], own[1]), jnp.where(line % 2 == 0, far[0], far[1])
    )
    out_ref[...] = rows.astype(bf16)


def slab_request(map_ref, slot):
    owners = map_ref[...]
    place = iota(owners.shape, 1) // SLABS_REQ
    return jnp.sum(jnp.where(owners == slot, place, 0), axis=1, keepdims=True)


def attend_kernel(
    idx_ref,
    lengths_ref,
    got_ref,
    w_uk_ref,
    slab_ref,
    slab_pos_ref,
    map_ref,
    keep_ref,
    give_ref,
):
    holder = idx_ref[0]
    core = holder % CORES
    req_v = slab_request(map_ref, holder)
    req = jnp.sum(req_v)

    shape = (2 * HEADS, got_ref.shape[0])
    part = iota(shape, 0)
    want = (req_v * HEADS + part % HEADS) * 2 + part // HEADS
    pick = jnp.where(iota(shape, 1) == want, 1.0, 0.0).astype(bf16)
    q_all = nn_dot(pick, got_ref[...]).astype(bf16)
    rope_dim = slab_ref.shape[2] - LATENT
    q_nope, q_rope = q_all[:HEADS], q_all[HEADS:, :rope_dim]

    wide = jnp.concatenate([q_nope] * HEADS, axis=1)
    diagonal = iota(wide.shape, 1) // NOPE == iota(wide.shape, 0)
    wide = jnp.where(diagonal, wide, jnp.zeros_like(wide))
    w_uk = w_uk_ref[0].reshape(wide.shape[1], LATENT)
    q_lat = nn_dot(wide, w_uk).astype(bf16)

    latent = slab_ref[0, 0, :LATENT]
    rotary = slab_ref[0, 0, LATENT:]
    score = (nn_dot(q_lat, latent) + nn_dot(q_rope, rotary)) * score_scale
    live = slab_pos_ref[0] < lengths_ref[req]
    top = jnp.max(jnp.where(live, score, neg_fill), axis=1, keepdims=True)
    weight = jnp.where(live, jnp.exp(jnp.where(live, score - top, 0.0)), 0.0).astype(bf16)
    total = jnp.sum(weight.astype(f32), axis=1, keepdims=True)
    safe = jnp.where(total > 0.0, total, 1.0)
    out = nt_dot(weight, latent) / safe
    level = jnp.where(total > 0.0, top + jnp.log(safe), neg_fill)

    blocks = [out[:, j * LANES : (j + 1) * LANES].astype(bf16) for j in range(CHUNKS)]
    blocks += pieces(jnp.broadcast_to(level, (HEADS, LANES)))
    stacked = jnp.concatenate(blocks, axis=0)
    shape = (HEADS * MSG, stacked.shape[0])
    line, column = iota(shape, 0), iota(shape, 1)
    half = HEADS // CORES * MSG
    parity = jnp.where(line < half, core, 1 - core)
    head = line % half // MSG * CORES + parity
    wanted = (column == line % MSG * HEADS + head) & (line % MSG < len(blocks))
    spread = jnp.where(wanted, 1.0, 0.0).astype(bf16)
    message = nn_dot(spread, stacked).astype(bf16)
    keep_ref[...] = message[:half]
    give_ref[...] = message[half:]


def own_kernel(
    idx_ref,
    lengths_ref,
    query_ref,
    w_uk_ref,
    w_uv_ref,
    newlat_ref,
    map_ref,
    deep_ref,
    deep_pos_ref,
    aux_ref,
):
    holder = idx_ref[0]
    own_req = holder // HEADS
    own_head = holder % HEADS
    nope, rope = query_ref[0, :, :NOPE], query_ref[0, :, NOPE:]

    own_lat = nn_dot(nope[:1], w_uk_ref[0, own_head]).astype(bf16).astype(f32)
    newlat = picked_row(newlat_ref[0], own_req)
    own_score = (
        jnp.sum(own_lat * newlat[:, :LATENT], axis=1, keepdims=True)
        + jnp.sum(rope[:1].astype(f32) * newlat[:, LATENT:], axis=1, keepdims=True)
    ) * score_scale
    for j in range(CHUNKS):
        aux_ref[j : j + 1, :] = newlat[:, j * LANES : (j + 1) * LANES]
    aux_ref[CHUNKS : CHUNKS + 1, :] = jnp.broadcast_to(own_score, (1, LANES))

    own_lat = nn_dot(nope[1:], w_uk_ref[1, own_head]).astype(bf16)
    latent = deep_ref[0, own_req, :LATENT]
    rotary = deep_ref[0, own_req, LATENT:]
    score = (nn_dot(own_lat, latent) + nn_dot(rope[1:], rotary)) * score_scale
    live = deep_pos_ref[0, pl.ds(own_req, 1), :] < lengths_ref[own_req]
    block_max = jnp.max(jnp.where(live, score, neg_fill), axis=1, keepdims=True)
    weight = jnp.where(live, jnp.exp(jnp.where(live, score - block_max, 0.0)), 0.0).astype(bf16)
    block_sum = jnp.sum(weight.astype(f32), axis=1, keepdims=True)
    block_out = nt_dot(weight, latent)
    newlat = picked_row(newlat_ref[1], own_req)
    own_score = (
        jnp.sum(own_lat.astype(f32) * newlat[:, :LATENT], axis=1, keepdims=True)
        + jnp.sum(rope[1:].astype(f32) * newlat[:, LATENT:], axis=1, keepdims=True)
    ) * score_scale
    top = jnp.maximum(own_score, block_max)
    own_factor = jnp.exp(own_score - top)
    far_factor = jnp.exp(block_max - top)
    total = own_factor + block_sum * far_factor
    mixed = ((own_factor * newlat[:, :LATENT] + block_out * far_factor) / total).astype(bf16)
    aux_ref[CHUNKS + 1 : CHUNKS + 2, :] = nn_dot(mixed, w_uv_ref[1, own_head])

    for row, slot in ((CHUNKS + 2, holder), (CHUNKS + 3, holder + 1 - 2 * (holder % CORES))):
        req = slab_request(map_ref, slot).astype(f32)
        aux_ref[row : row + 1, :] = jnp.broadcast_to(req, (1, LANES))


def merge_kernel(keep_ref, far_ref, aux_ref, send_ref):
    near_req, far_req = aux_ref[CHUNKS + 2 : CHUNKS + 3, :], aux_ref[CHUNKS + 3 : CHUNKS + 4, :]
    blocks = keep_ref.shape[0] // MSG
    near = keep_ref[...].astype(f32).reshape(blocks, MSG, LANES)
    far = far_ref[...].astype(f32).reshape(blocks, MSG, LANES)
    near_level, far_level = message_level(near), message_level(far)
    top = jnp.maximum(near_level, far_level)
    near_factor, far_factor = jnp.exp(near_level - top), jnp.exp(far_level - top)
    total = near_factor + far_factor
    merged = (near_factor * near + far_factor * far) / total
    level = top + (jnp.log(total) - LOG_2)
    line = iota(merged.shape, 1)
    for j, piece in enumerate(pieces(level)):
        merged = jnp.where(line == CHUNKS + j, piece.astype(f32), merged)
    same = near_req == far_req
    near = jnp.where(same, merged, near).reshape(keep_ref.shape)
    far = jnp.where(same, merged, far).reshape(keep_ref.shape)
    rows = keep_ref.shape[0]
    for b in range(send_ref.shape[0] // rows):
        send_ref[b * rows : (b + 1) * rows, :] = jnp.where(near_req == b, near, far).astype(bf16)


def combine_kernel(idx_ref, map_ref, got_ref, aux_ref, w_uv_ref, out_ref):
    holder = idx_ref[0]
    own_req = holder // HEADS
    own_head = holder % HEADS
    own = aux_ref[...]
    own_score = own[CHUNKS : CHUNKS + 1]
    messages, levels = [], []
    top = own_score
    for s in range(SLABS_REQ):
        chip = map_ref[0, own_req * SLABS_REQ + s] // CORES
        message = got_ref[pl.ds(pl.multiple_of(chip * MSG, MSG), MSG), :].astype(f32)
        level = message_level(message)
        messages.append(message)
        levels.append(level)
        top = jnp.maximum(top, level)
    total = jnp.exp(own_score - top)
    mixed = total * own
    for message, level in zip(messages, levels):
        factor = jnp.exp(level - top)
        total = total + factor
        mixed = mixed + factor * message
    mixed = (mixed / total).astype(bf16).astype(f32)
    row = jnp.concatenate([mixed[j : j + 1] for j in range(CHUNKS)], axis=1).astype(bf16)
    out = jnp.concatenate([nn_dot(row, w_uv_ref[0, own_head]), own[CHUNKS + 1 : CHUNKS + 2]], axis=0)
    out_ref[0] = out.astype(bf16)


VMEM = pl.BlockSpec(memory_space=pltpu.VMEM)
SMEM = pl.BlockSpec(memory_space=pltpu.SMEM)


def call(kernel, out_shape, in_specs, flops):
    many = isinstance(out_shape, tuple)
    return pl.pallas_call(
        kernel,
        out_shape=out_shape,
        in_specs=in_specs,
        out_specs=(VMEM,) * len(out_shape) if many else VMEM,
        compiler_params=pltpu.CompilerParams(vmem_limit_bytes=12 << 20),
        cost_estimate=pl.CostEstimate(flops=flops, bytes_accessed=1 << 20, transcendentals=0),
    )


def exchanged(rows, per_chip):
    chips = lax.axis_size("chips")
    tiles = rows.reshape(chips, per_chip, LANES)
    return lax.all_to_all(tiles, "chips", 0, 0, tiled=True).reshape(rows.shape)


def swapped(x):
    return lax.ppermute(x, "cores", [(k, (k + 1) % CORES) for k in range(CORES)])


def shards(
    q_nope,
    q_rope,
    w_uk,
    w_uv,
    new_latent,
    shallow_cache,
    slot_positions,
    slab_map,
    deep_cache,
    deep_positions,
    lengths,
):
    chips = lax.axis_size("chips")
    holder = lax.axis_index("chips") * CORES + lax.axis_index("cores")
    holder = holder.astype(jnp.int32).reshape(1)
    shape = jax.ShapeDtypeStruct
    q_nope, q_rope = q_nope.swapaxes(0, 1), q_rope.swapaxes(0, 1)
    shallow_cache, deep_cache = shallow_cache.swapaxes(2, 3), deep_cache.swapaxes(2, 3)
    far_nope, far_rope = swapped(q_nope), swapped(q_rope)
    query = jnp.concatenate([q_nope, q_rope], axis=-1)
    queries = call(
        prep_kernel, shape((chips * CORES * 2, LANES), bf16), [SMEM] + [VMEM] * 3, 1 << 33
    )(holder, query, far_nope, far_rope)
    queries = exchanged(queries, CORES * 2)
    block = shape((HEADS // CORES * MSG, LANES), bf16)
    keep, give = call(attend_kernel, (block, block), [SMEM, SMEM] + [VMEM] * 5, 1 << 24)(
        holder, lengths, queries, w_uk, shallow_cache, slot_positions, slab_map
    )
    far = swapped(give)
    aux = call(own_kernel, shape((MSG, LANES), f32), [SMEM, SMEM] + [VMEM] * 7, 1 << 24)(
        holder, lengths, query, w_uk, w_uv, new_latent, slab_map, deep_cache, deep_positions
    )
    partials = call(merge_kernel, shape((chips * MSG, LANES), bf16), [VMEM] * 3, 1 << 20)(
        keep, far, aux
    )
    partials = exchanged(partials, MSG)
    rows = call(combine_kernel, shape(q_nope.shape, bf16), [SMEM, SMEM] + [VMEM] * 3, 1 << 20)(
        holder, slab_map, partials, aux, w_uv
    )
    return rows.swapaxes(0, 1)


def solution(mesh):
    groups, holders = mesh.shape["groups"], mesh.shape["holders"]
    mesh = Mesh(
        mesh.devices.reshape(groups, holders // CORES, CORES), ("groups", "chips", "cores")
    )
    spread = ("groups", "chips", "cores")
    in_specs = (
        P(None, spread, None),
        P(None, spread, None),
        P(),
        P(),
        P(None, "groups", None),
        P(None, spread, None, None),
        P(None, spread, None),
        P(None, "groups"),
        P(None, "groups", None, None),
        P(None, "groups", None),
        P("groups"),
    )
    return jax.shard_map(
        shards, mesh=mesh, in_specs=in_specs, out_specs=P(None, spread, None), check_vma=False
    )
```

```python
import math

import jax
import jax.numpy as jnp
from jax import lax
from jax.experimental import pallas as pl
from jax.experimental.pallas import tpu as pltpu
from jax.sharding import Mesh
from jax.sharding import PartitionSpec as P

HEADS = 16
LATENT = 512
NOPE = 128
SLABS_REQ = 16
LANES = 128
CHUNKS = LATENT // LANES
MSG = 8
CORES = 2
LOG_2 = math.log(2.0)

score_scale = 192.0 ** (-0.5)
neg_fill = -1e30
f32 = jnp.float32
bf16 = jnp.bfloat16


def iota(shape, dim):
    return lax.broadcasted_iota(jnp.int32, shape, dim)


def nt_dot(a, b):
    return lax.dot_general(a, b, (((1,), (1,)), ((), ())), preferred_element_type=f32)


def nn_dot(a, b):
    return jnp.dot(a, b, preferred_element_type=f32)


def picked_row(rows, at):
    rows = rows.astype(f32)
    return jnp.sum(jnp.where(iota(rows.shape, 0) == at, rows, 0.0), axis=0, keepdims=True)


def pieces(x):
    out = []
    for _ in range(3):
        out.append(x.astype(bf16))
        x = x - out[-1].astype(f32)
    return out


def message_level(message):
    rows = [message[..., CHUNKS + j : CHUNKS + j + 1, :] for j in range(3)]
    return rows[0] + (rows[1] + rows[2])


def prep_kernel(idx_ref, query_ref, far_nope_ref, far_rope_ref, out_ref):
    first = idx_ref[0] % CORES == 0

    def padded(row):
        row = row.astype(f32)
        return jnp.concatenate([row, jnp.zeros((1, LANES - row.shape[1]), f32)], axis=1)

    own = query_ref[0, :1, :NOPE].astype(f32), padded(query_ref[0, :1, NOPE:])
    far = far_nope_ref[0, :1].astype(f32), padded(far_rope_ref[0, :1])
    shape = (out_ref.shape[0], LANES)
    line = iota(shape, 0) % (2 * CORES)
    near = (line < 2) == first
    rows = jnp.where(
        near, jnp.where(line % 2 == 0, own[0], own[1]), jnp.where(line % 2 == 0, far[0], far[1])
    )
    out_ref[...] = rows.astype(bf16)


def slab_request(map_ref, slot):
    owners = map_ref[...]
    place = iota(owners.shape, 1) // SLABS_REQ
    return jnp.sum(jnp.where(owners == slot, place, 0), axis=1, keepdims=True)


def length_of(lengths_ref, req):
    lengths = lengths_ref[...]
    mine = jnp.where(iota(lengths.shape, 1) == req, lengths, 0)
    return jnp.sum(mine, axis=1, keepdims=True)


def attend_kernel(
    idx_ref,
    lengths_ref,
    got_ref,
    w_uk_ref,
    slab_ref,
    slab_pos_ref,
    map_ref,
    deep_hbm,
    w_uv_hbm,
    keep_ref,
    give_ref,
    deep_ref,
    w_up_ref,
    sems,
):
    holder = idx_ref[0]
    core = holder % CORES
    copies = [
        pltpu.make_async_copy(deep_hbm.at[0, holder // HEADS], deep_ref, sems.at[0]),
        pltpu.make_async_copy(w_uv_hbm.at[0, holder % HEADS], w_up_ref.at[0], sems.at[1]),
        pltpu.make_async_copy(w_uv_hbm.at[1, holder % HEADS], w_up_ref.at[1], sems.at[2]),
    ]
    for copy in copies:
        copy.start()
    req_v = slab_request(map_ref, holder)

    shape = (2 * HEADS, got_ref.shape[0])
    part = iota(shape, 0)
    want = (req_v * HEADS + part % HEADS) * 2 + part // HEADS
    pick = jnp.where(iota(shape, 1) == want, 1.0, 0.0).astype(bf16)
    q_all = nn_dot(pick, got_ref[...]).astype(bf16)
    rope_dim = slab_ref.shape[2] - LATENT
    q_nope, q_rope = q_all[:HEADS], q_all[HEADS:, :rope_dim]

    wide = jnp.concatenate([q_nope] * HEADS, axis=1)
    diagonal = iota(wide.shape, 1) // NOPE == iota(wide.shape, 0)
    wide = jnp.where(diagonal, wide, jnp.zeros_like(wide))
    w_uk = w_uk_ref[0].reshape(wide.shape[1], LATENT)
    q_lat = nn_dot(wide, w_uk).astype(bf16)

    latent = slab_ref[0, 0, :LATENT]
    rotary = slab_ref[0, 0, LATENT:]
    score = (nn_dot(q_lat, latent) + nn_dot(q_rope, rotary)) * score_scale
    live = slab_pos_ref[0] < length_of(lengths_ref, req_v)
    top = jnp.max(jnp.where(live, score, neg_fill), axis=1, keepdims=True)
    weight = jnp.where(live, jnp.exp(jnp.where(live, score - top, 0.0)), 0.0).astype(bf16)
    total = jnp.sum(weight.astype(f32), axis=1, keepdims=True)
    safe = jnp.where(total > 0.0, total, 1.0)
    out = nt_dot(weight, latent) / safe
    level = jnp.where(total > 0.0, top + jnp.log(safe), neg_fill)

    blocks = [out[:, j * LANES : (j + 1) * LANES].astype(bf16) for j in range(CHUNKS)]
    blocks += pieces(jnp.broadcast_to(level, (HEADS, LANES)))
    stacked = jnp.concatenate(blocks, axis=0)
    shape = (HEADS * MSG, stacked.shape[0])
    line, column = iota(shape, 0), iota(shape, 1)
    half = HEADS // CORES * MSG
    parity = jnp.where(line < half, core, 1 - core)
    head = line % half // MSG * CORES + parity
    wanted = (column == line % MSG * HEADS + head) & (line % MSG < len(blocks))
    spread = jnp.where(wanted, 1.0, 0.0).astype(bf16)
    message = nn_dot(spread, stacked).astype(bf16)
    keep_ref[...] = message[:half]
    give_ref[...] = message[half:]
    for copy in copies:
        copy.wait()


def own_kernel(
    idx_ref,
    lengths_ref,
    query_ref,
    w_uk_ref,
    w_up_ref,
    newlat_ref,
    map_ref,
    deep_ref,
    deep_pos_ref,
    aux_ref,
    chips_ref,
):
    holder = idx_ref[0]
    own_req = holder // HEADS
    own_head = holder % HEADS
    nope, rope = query_ref[0, :, :NOPE], query_ref[0, :, NOPE:]

    own_lat = nn_dot(nope[:1], w_uk_ref[0, own_head]).astype(bf16).astype(f32)
    newlat = picked_row(newlat_ref[0], own_req)
    own_score = (
        jnp.sum(own_lat * newlat[:, :LATENT], axis=1, keepdims=True)
        + jnp.sum(rope[:1].astype(f32) * newlat[:, LATENT:], axis=1, keepdims=True)
    ) * score_scale
    for j in range(CHUNKS):
        aux_ref[j : j + 1, :] = newlat[:, j * LANES : (j + 1) * LANES]
    aux_ref[CHUNKS : CHUNKS + 1, :] = jnp.broadcast_to(own_score, (1, LANES))

    own_lat = nn_dot(nope[1:], w_uk_ref[1, own_head]).astype(bf16)
    latent = deep_ref[:LATENT]
    rotary = deep_ref[LATENT:]
    score = (nn_dot(own_lat, latent) + nn_dot(rope[1:], rotary)) * score_scale
    live = deep_pos_ref[0, pl.ds(own_req, 1), :] < length_of(lengths_ref, own_req)
    block_max = jnp.max(jnp.where(live, score, neg_fill), axis=1, keepdims=True)
    weight = jnp.where(live, jnp.exp(jnp.where(live, score - block_max, 0.0)), 0.0).astype(bf16)
    block_sum = jnp.sum(weight.astype(f32), axis=1, keepdims=True)
    block_out = nt_dot(weight, latent)
    newlat = picked_row(newlat_ref[1], own_req)
    own_score = (
        jnp.sum(own_lat.astype(f32) * newlat[:, :LATENT], axis=1, keepdims=True)
        + jnp.sum(rope[1:].astype(f32) * newlat[:, LATENT:], axis=1, keepdims=True)
    ) * score_scale
    top = jnp.maximum(own_score, block_max)
    own_factor = jnp.exp(own_score - top)
    far_factor = jnp.exp(block_max - top)
    total = own_factor + block_sum * far_factor
    mixed = ((own_factor * newlat[:, :LATENT] + block_out * far_factor) / total).astype(bf16)
    aux_ref[CHUNKS + 1 : CHUNKS + 2, :] = nn_dot(mixed, w_up_ref[1])

    for row, slot in ((CHUNKS + 2, holder), (CHUNKS + 3, holder + 1 - 2 * (holder % CORES))):
        req = slab_request(map_ref, slot).astype(f32)
        aux_ref[row : row + 1, :] = jnp.broadcast_to(req, (1, LANES))

    shape = chips_ref.shape
    place = iota(shape, 1) == own_req * SLABS_REQ + iota(shape, 0)
    slots = jnp.sum(jnp.where(place, map_ref[...], 0), axis=1, keepdims=True)
    chips_ref[...] = jnp.broadcast_to(slots // CORES, shape)


def merge_kernel(keep_ref, far_ref, aux_ref, send_ref):
    near_req, far_req = aux_ref[CHUNKS + 2 : CHUNKS + 3, :], aux_ref[CHUNKS + 3 : CHUNKS + 4, :]
    blocks = keep_ref.shape[0] // MSG
    near = keep_ref[...].astype(f32).reshape(blocks, MSG, LANES)
    far = far_ref[...].astype(f32).reshape(blocks, MSG, LANES)
    near_level, far_level = message_level(near), message_level(far)
    top = jnp.maximum(near_level, far_level)
    near_factor, far_factor = jnp.exp(near_level - top), jnp.exp(far_level - top)
    total = near_factor + far_factor
    merged = (near_factor * near + far_factor * far) / total
    level = top + (jnp.log(total) - LOG_2)
    line = iota(merged.shape, 1)
    for j, piece in enumerate(pieces(level)):
        merged = jnp.where(line == CHUNKS + j, piece.astype(f32), merged)
    same = near_req == far_req
    near = jnp.where(same, merged, near).reshape(keep_ref.shape)
    far = jnp.where(same, merged, far).reshape(keep_ref.shape)
    rows = keep_ref.shape[0]
    for b in range(send_ref.shape[0] // rows):
        send_ref[b * rows : (b + 1) * rows, :] = jnp.where(near_req == b, near, far).astype(bf16)


def combine_kernel(chips_ref, got_ref, aux_ref, w_up_ref, out_ref):
    own = aux_ref[...]
    chips = chips_ref[...]
    own_score = own[CHUNKS : CHUNKS + 1]
    messages, levels = [], []
    top = own_score
    for s in range(SLABS_REQ):
        chip = chips[s, 0]
        message = got_ref[pl.ds(pl.multiple_of(chip * MSG, MSG), MSG), :].astype(f32)
        level = message_level(message)
        messages.append(message)
        levels.append(level)
        top = jnp.maximum(top, level)
    total = jnp.exp(own_score - top)
    mixed = total * own
    for message, level in zip(messages, levels):
        factor = jnp.exp(level - top)
        total = total + factor
        mixed = mixed + factor * message
    mixed = (mixed / total).astype(bf16).astype(f32)
    row = jnp.concatenate([mixed[j : j + 1] for j in range(CHUNKS)], axis=1).astype(bf16)
    out = jnp.concatenate([nn_dot(row, w_up_ref[0]), own[CHUNKS + 1 : CHUNKS + 2]], axis=0)
    out_ref[0] = out.astype(bf16)


VMEM = pl.BlockSpec(memory_space=pltpu.VMEM)
SMEM = pl.BlockSpec(memory_space=pltpu.SMEM)
ANY = pl.BlockSpec(memory_space=pl.ANY)


def call(kernel, out_shape, in_specs, flops, scratch_shapes=()):
    many = isinstance(out_shape, tuple)
    return pl.pallas_call(
        kernel,
        out_shape=out_shape,
        in_specs=in_specs,
        out_specs=(VMEM,) * len(out_shape) if many else VMEM,
        scratch_shapes=scratch_shapes,
        compiler_params=pltpu.CompilerParams(vmem_limit_bytes=12 << 20),
        cost_estimate=pl.CostEstimate(flops=flops, bytes_accessed=1 << 20, transcendentals=0),
    )


def exchanged(rows, per_chip):
    chips = lax.axis_size("chips")
    tiles = rows.reshape(chips, per_chip, LANES)
    return lax.all_to_all(tiles, "chips", 0, 0, tiled=True).reshape(rows.shape)


def swapped(x):
    return lax.ppermute(x, "cores", [(k, (k + 1) % CORES) for k in range(CORES)])


def shards(
    q_nope,
    q_rope,
    w_uk,
    w_uv,
    new_latent,
    shallow_cache,
    slot_positions,
    slab_map,
    deep_cache,
    deep_positions,
    lengths,
):
    chips = lax.axis_size("chips")
    holder = lax.axis_index("chips") * CORES + lax.axis_index("cores")
    holder = holder.astype(jnp.int32).reshape(1)
    shape = jax.ShapeDtypeStruct
    q_nope, q_rope = q_nope.swapaxes(0, 1), q_rope.swapaxes(0, 1)
    shallow_cache, deep_cache = shallow_cache.swapaxes(2, 3), deep_cache.swapaxes(2, 3)
    far_nope, far_rope = swapped(q_nope), swapped(q_rope)
    query = jnp.concatenate([q_nope, q_rope], axis=-1)
    queries = call(
        prep_kernel, shape((chips * CORES * 2, LANES), bf16), [SMEM] + [VMEM] * 3, 1 << 33
    )(holder, query, far_nope, far_rope)
    queries = exchanged(queries, CORES * 2)
    block = shape((HEADS // CORES * MSG, LANES), bf16)
    lengths = lengths.reshape(1, -1)
    keep, give, deep, w_up = call(
        attend_kernel,
        (
            block,
            block,
            shape(deep_cache.shape[2:], bf16),
            shape((w_uv.shape[0], *w_uv.shape[2:]), bf16),
        ),
        [SMEM] + [VMEM] * 6 + [ANY] * 2,
        1 << 24,
        [pltpu.SemaphoreType.DMA((3,))],
    )(
        holder,
        lengths,
        queries,
        w_uk,
        shallow_cache,
        slot_positions,
        slab_map,
        pltpu.with_memory_space_constraint(deep_cache, pltpu.HBM),
        pltpu.with_memory_space_constraint(w_uv, pltpu.HBM),
    )
    far = swapped(give)
    aux, slab_chips = call(
        own_kernel,
        (shape((MSG, LANES), f32), shape((SLABS_REQ, LANES), jnp.int32)),
        [SMEM] + [VMEM] * 8,
        1 << 24,
    )(holder, lengths, query, w_uk, w_up, new_latent, slab_map, deep, deep_positions)
    partials = call(merge_kernel, shape((chips * MSG, LANES), bf16), [VMEM] * 3, 1 << 20)(
        keep, far, aux
    )
    partials = exchanged(partials, MSG)
    rows = call(combine_kernel, shape(q_nope.shape, bf16), [VMEM] * 4, 1 << 20)(
        slab_chips, partials, aux, w_up
    )
    return rows.swapaxes(0, 1)


def solution(mesh):
    groups, holders = mesh.shape["groups"], mesh.shape["holders"]
    mesh = Mesh(
        mesh.devices.reshape(groups, holders // CORES, CORES), ("groups", "chips", "cores")
    )
    spread = ("groups", "chips", "cores")
    in_specs = (
        P(None, spread, None),
        P(None, spread, None),
        P(),
        P(),
        P(None, "groups", None),
        P(None, spread, None, None),
        P(None, spread, None),
        P(None, "groups"),
        P(None, "groups", None, None),
        P(None, "groups", None),
        P("groups"),
    )
    return jax.shard_map(
        shards, mesh=mesh, in_specs=in_specs, out_specs=P(None, spread, None), check_vma=False
    )
```

```python
import math

import jax
import jax.numpy as jnp
from jax import lax
from jax.experimental import pallas as pl
from jax.experimental.pallas import tpu as pltpu
from jax.sharding import Mesh
from jax.sharding import PartitionSpec as P

HEADS = 16
LATENT = 512
NOPE = 128
SLABS_REQ = 16
LANES = 128
CHUNKS = LATENT // LANES
MSG = 8
CORES = 2
LOG_2 = math.log(2.0)

score_scale = 192.0 ** (-0.5)
neg_fill = -1e30
f32 = jnp.float32
bf16 = jnp.bfloat16


def iota(shape, dim):
    return lax.broadcasted_iota(jnp.int32, shape, dim)


def nt_dot(a, b):
    return lax.dot_general(a, b, (((1,), (1,)), ((), ())), preferred_element_type=f32)


def nn_dot(a, b):
    return jnp.dot(a, b, preferred_element_type=f32)


def picked_row(rows, at):
    rows = rows.astype(f32)
    return jnp.sum(jnp.where(iota(rows.shape, 0) == at, rows, 0.0), axis=0, keepdims=True)


def pieces(x):
    out = []
    for _ in range(3):
        out.append(x.astype(bf16))
        x = x - out[-1].astype(f32)
    return out


def message_level(message):
    rows = [message[..., CHUNKS + j : CHUNKS + j + 1, :] for j in range(3)]
    return rows[0] + (rows[1] + rows[2])


def prep_kernel(idx_ref, query_ref, far_nope_ref, far_rope_ref, out_ref):
    first = idx_ref[0] % CORES == 0

    def padded(row):
        row = row.astype(f32)
        return jnp.concatenate([row, jnp.zeros((1, LANES - row.shape[1]), f32)], axis=1)

    own = query_ref[0, :1, :NOPE].astype(f32), padded(query_ref[0, :1, NOPE:])
    far = far_nope_ref[0, :1].astype(f32), padded(far_rope_ref[0, :1])
    shape = (out_ref.shape[0], LANES)
    line = iota(shape, 0) % (2 * CORES)
    near = (line < 2) == first
    rows = jnp.where(
        near, jnp.where(line % 2 == 0, own[0], own[1]), jnp.where(line % 2 == 0, far[0], far[1])
    )
    out_ref[...] = rows.astype(bf16)


def slab_request(map_ref, slot):
    owners = map_ref[...]
    place = iota(owners.shape, 1) // SLABS_REQ
    return jnp.sum(jnp.where(owners == slot, place, 0), axis=1, keepdims=True)


def length_of(lengths_ref, req):
    lengths = lengths_ref[...]
    mine = jnp.where(iota(lengths.shape, 1) == req, lengths, 0)
    return jnp.sum(mine, axis=1, keepdims=True)


def attend_kernel(
    idx_ref,
    lengths_ref,
    got_ref,
    w_uk_ref,
    slab_ref,
    slab_pos_ref,
    map_ref,
    keep_ref,
    give_ref,
):
    holder = idx_ref[0]
    core = holder % CORES
    req_v = slab_request(map_ref, holder)

    shape = (2 * HEADS, got_ref.shape[0])
    part = iota(shape, 0)
    want = (req_v * HEADS + part % HEADS) * 2 + part // HEADS
    pick = jnp.where(iota(shape, 1) == want, 1.0, 0.0).astype(bf16)
    q_all = nn_dot(pick, got_ref[...]).astype(bf16)
    rope_dim = slab_ref.shape[2] - LATENT
    q_nope, q_rope = q_all[:HEADS], q_all[HEADS:, :rope_dim]

    wide = jnp.concatenate([q_nope] * HEADS, axis=1)
    diagonal = iota(wide.shape, 1) // NOPE == iota(wide.shape, 0)
    wide = jnp.where(diagonal, wide, jnp.zeros_like(wide))
    w_uk = w_uk_ref[0].reshape(wide.shape[1], LATENT)
    q_lat = nn_dot(wide, w_uk).astype(bf16)

    latent = slab_ref[0, 0, :LATENT]
    rotary = slab_ref[0, 0, LATENT:]
    score = (nn_dot(q_lat, latent) + nn_dot(q_rope, rotary)) * score_scale
    live = slab_pos_ref[0] < length_of(lengths_ref, req_v)
    top = jnp.max(jnp.where(live, score, neg_fill), axis=1, keepdims=True)
    weight = jnp.where(live, jnp.exp(jnp.where(live, score - top, 0.0)), 0.0).astype(bf16)
    total = jnp.sum(weight.astype(f32), axis=1, keepdims=True)
    safe = jnp.where(total > 0.0, total, 1.0)
    out = nt_dot(weight, latent) / safe
    level = jnp.where(total > 0.0, top + jnp.log(safe), neg_fill)

    blocks = [out[:, j * LANES : (j + 1) * LANES].astype(bf16) for j in range(CHUNKS)]
    blocks += pieces(jnp.broadcast_to(level, (HEADS, LANES)))
    stacked = jnp.concatenate(blocks, axis=0)
    shape = (HEADS * MSG, stacked.shape[0])
    line, column = iota(shape, 0), iota(shape, 1)
    half = HEADS // CORES * MSG
    parity = jnp.where(line < half, core, 1 - core)
    head = line % half // MSG * CORES + parity
    wanted = (column == line % MSG * HEADS + head) & (line % MSG < len(blocks))
    spread = jnp.where(wanted, 1.0, 0.0).astype(bf16)
    message = nn_dot(spread, stacked).astype(bf16)
    keep_ref[...] = message[:half]
    give_ref[...] = message[half:]


def own_kernel(
    idx_ref,
    lengths_ref,
    query_ref,
    w_uk_ref,
    w_uv_ref,
    newlat_ref,
    map_ref,
    deep_ref,
    deep_pos_ref,
    aux_ref,
    chips_ref,
):
    holder = idx_ref[0]
    own_req = holder // HEADS
    own_head = holder % HEADS
    nope, rope = query_ref[0, :, :NOPE], query_ref[0, :, NOPE:]

    own_lat = nn_dot(nope[:1], w_uk_ref[0, own_head]).astype(bf16).astype(f32)
    newlat = picked_row(newlat_ref[0], own_req)
    own_score = (
        jnp.sum(own_lat * newlat[:, :LATENT], axis=1, keepdims=True)
        + jnp.sum(rope[:1].astype(f32) * newlat[:, LATENT:], axis=1, keepdims=True)
    ) * score_scale
    for j in range(CHUNKS):
        aux_ref[j : j + 1, :] = newlat[:, j * LANES : (j + 1) * LANES]
    aux_ref[CHUNKS : CHUNKS + 1, :] = jnp.broadcast_to(own_score, (1, LANES))

    own_lat = nn_dot(nope[1:], w_uk_ref[1, own_head]).astype(bf16)
    latent = deep_ref[0, own_req, :LATENT]
    rotary = deep_ref[0, own_req, LATENT:]
    score = (nn_dot(own_lat, latent) + nn_dot(rope[1:], rotary)) * score_scale
    live = deep_pos_ref[0, pl.ds(own_req, 1), :] < length_of(lengths_ref, own_req)
    block_max = jnp.max(jnp.where(live, score, neg_fill), axis=1, keepdims=True)
    weight = jnp.where(live, jnp.exp(jnp.where(live, score - block_max, 0.0)), 0.0).astype(bf16)
    block_sum = jnp.sum(weight.astype(f32), axis=1, keepdims=True)
    block_out = nt_dot(weight, latent)
    newlat = picked_row(newlat_ref[1], own_req)
    own_score = (
        jnp.sum(own_lat.astype(f32) * newlat[:, :LATENT], axis=1, keepdims=True)
        + jnp.sum(rope[1:].astype(f32) * newlat[:, LATENT:], axis=1, keepdims=True)
    ) * score_scale
    top = jnp.maximum(own_score, block_max)
    own_factor = jnp.exp(own_score - top)
    far_factor = jnp.exp(block_max - top)
    total = own_factor + block_sum * far_factor
    mixed = ((own_factor * newlat[:, :LATENT] + block_out * far_factor) / total).astype(bf16)
    aux_ref[CHUNKS + 1 : CHUNKS + 2, :] = nn_dot(mixed, w_uv_ref[1, own_head])

    for row, slot in ((CHUNKS + 2, holder), (CHUNKS + 3, holder + 1 - 2 * (holder % CORES))):
        req = slab_request(map_ref, slot).astype(f32)
        aux_ref[row : row + 1, :] = jnp.broadcast_to(req, (1, LANES))

    shape = chips_ref.shape
    place = iota(shape, 1) == own_req * SLABS_REQ + iota(shape, 0)
    slots = jnp.sum(jnp.where(place, map_ref[...], 0), axis=1, keepdims=True)
    chips_ref[...] = jnp.broadcast_to(slots // CORES, shape)


def merge_kernel(keep_ref, far_ref, aux_ref, send_ref):
    near_req, far_req = aux_ref[CHUNKS + 2 : CHUNKS + 3, :], aux_ref[CHUNKS + 3 : CHUNKS + 4, :]
    blocks = keep_ref.shape[0] // MSG
    near = keep_ref[...].astype(f32).reshape(blocks, MSG, LANES)
    far = far_ref[...].astype(f32).reshape(blocks, MSG, LANES)
    near_level, far_level = message_level(near), message_level(far)
    top = jnp.maximum(near_level, far_level)
    near_factor, far_factor = jnp.exp(near_level - top), jnp.exp(far_level - top)
    total = near_factor + far_factor
    merged = (near_factor * near + far_factor * far) / total
    level = top + (jnp.log(total) - LOG_2)
    line = iota(merged.shape, 1)
    for j, piece in enumerate(pieces(level)):
        merged = jnp.where(line == CHUNKS + j, piece.astype(f32), merged)
    same = near_req == far_req
    near = jnp.where(same, merged, near).reshape(keep_ref.shape)
    far = jnp.where(same, merged, far).reshape(keep_ref.shape)
    rows = keep_ref.shape[0]
    for b in range(send_ref.shape[0] // rows):
        send_ref[b * rows : (b + 1) * rows, :] = jnp.where(near_req == b, near, far).astype(bf16)


def combine_kernel(idx_ref, chips_ref, got_ref, aux_ref, w_uv_ref, out_ref):
    own_head = idx_ref[0] % HEADS
    own = aux_ref[...]
    chips = chips_ref[...]
    own_score = own[CHUNKS : CHUNKS + 1]
    messages, levels = [], []
    top = own_score
    for s in range(SLABS_REQ):
        chip = chips[s, 0]
        message = got_ref[pl.ds(pl.multiple_of(chip * MSG, MSG), MSG), :].astype(f32)
        level = message_level(message)
        messages.append(message)
        levels.append(level)
        top = jnp.maximum(top, level)
    total = jnp.exp(own_score - top)
    mixed = total * own
    for message, level in zip(messages, levels):
        factor = jnp.exp(level - top)
        total = total + factor
        mixed = mixed + factor * message
    mixed = (mixed / total).astype(bf16).astype(f32)
    row = jnp.concatenate([mixed[j : j + 1] for j in range(CHUNKS)], axis=1).astype(bf16)
    out = jnp.concatenate([nn_dot(row, w_uv_ref[0, own_head]), own[CHUNKS + 1 : CHUNKS + 2]], axis=0)
    out_ref[0] = out.astype(bf16)


VMEM = pl.BlockSpec(memory_space=pltpu.VMEM)
SMEM = pl.BlockSpec(memory_space=pltpu.SMEM)


def call(kernel, out_shape, in_specs, flops):
    many = isinstance(out_shape, tuple)
    return pl.pallas_call(
        kernel,
        out_shape=out_shape,
        in_specs=in_specs,
        out_specs=(VMEM,) * len(out_shape) if many else VMEM,
        compiler_params=pltpu.CompilerParams(vmem_limit_bytes=12 << 20),
        cost_estimate=pl.CostEstimate(flops=flops, bytes_accessed=1 << 20, transcendentals=0),
    )


def exchanged(rows, per_chip):
    chips = lax.axis_size("chips")
    tiles = rows.reshape(chips, per_chip, LANES)
    return lax.all_to_all(tiles, "chips", 0, 0, tiled=True).reshape(rows.shape)


def swapped(x):
    return lax.ppermute(x, "cores", [(k, (k + 1) % CORES) for k in range(CORES)])


def shards(
    q_nope,
    q_rope,
    w_uk,
    w_uv,
    new_latent,
    shallow_cache,
    slot_positions,
    slab_map,
    deep_cache,
    deep_positions,
    lengths,
):
    chips = lax.axis_size("chips")
    holder = lax.axis_index("chips") * CORES + lax.axis_index("cores")
    holder = holder.astype(jnp.int32).reshape(1)
    shape = jax.ShapeDtypeStruct
    q_nope, q_rope = q_nope.swapaxes(0, 1), q_rope.swapaxes(0, 1)
    shallow_cache, deep_cache = shallow_cache.swapaxes(2, 3), deep_cache.swapaxes(2, 3)
    far_nope, far_rope = swapped(q_nope), swapped(q_rope)
    query = jnp.concatenate([q_nope, q_rope], axis=-1)
    queries = call(
        prep_kernel, shape((chips * CORES * 2, LANES), bf16), [SMEM] + [VMEM] * 3, 1 << 33
    )(holder, query, far_nope, far_rope)
    queries = exchanged(queries, CORES * 2)
    block = shape((HEADS // CORES * MSG, LANES), bf16)
    lengths = lengths.reshape(1, -1)
    keep, give = call(attend_kernel, (block, block), [SMEM] + [VMEM] * 6, 1 << 24)(
        holder, lengths, queries, w_uk, shallow_cache, slot_positions, slab_map
    )
    far = swapped(give)
    aux, slab_chips = call(
        own_kernel,
        (shape((MSG, LANES), f32), shape((SLABS_REQ, LANES), jnp.int32)),
        [SMEM] + [VMEM] * 8,
        1 << 24,
    )(
        holder, lengths, query, w_uk, w_uv, new_latent, slab_map, deep_cache, deep_positions
    )
    partials = call(merge_kernel, shape((chips * MSG, LANES), bf16), [VMEM] * 3, 1 << 20)(
        keep, far, aux
    )
    partials = exchanged(partials, MSG)
    rows = call(combine_kernel, shape(q_nope.shape, bf16), [SMEM] + [VMEM] * 4, 1 << 20)(
        holder, slab_chips, partials, aux, w_uv
    )
    return rows.swapaxes(0, 1)


def solution(mesh):
    groups, holders = mesh.shape["groups"], mesh.shape["holders"]
    mesh = Mesh(
        mesh.devices.reshape(groups, holders // CORES, CORES), ("groups", "chips", "cores")
    )
    spread = ("groups", "chips", "cores")
    in_specs = (
        P(None, spread, None),
        P(None, spread, None),
        P(),
        P(),
        P(None, "groups", None),
        P(None, spread, None, None),
        P(None, spread, None),
        P(None, "groups"),
        P(None, "groups", None, None),
        P(None, "groups", None),
        P("groups"),
    )
    return jax.shard_map(
        shards, mesh=mesh, in_specs=in_specs, out_specs=P(None, spread, None), check_vma=False
    )
```

```python
import math

import jax
import jax.numpy as jnp
from jax import lax
from jax.experimental import pallas as pl
from jax.experimental.pallas import tpu as pltpu
from jax.sharding import Mesh
from jax.sharding import PartitionSpec as P

HEADS = 16
LATENT = 512
NOPE = 128
SLABS_REQ = 16
LANES = 128
MSG = 2
CORES = 2
LOG_2 = math.log(2.0)

score_scale = 192.0 ** (-0.5)
neg_fill = -1e30
f32 = jnp.float32
bf16 = jnp.bfloat16


def iota(shape, dim):
    return lax.broadcasted_iota(jnp.int32, shape, dim)


def nt_dot(a, b):
    return lax.dot_general(a, b, (((1,), (1,)), ((), ())), preferred_element_type=f32)


def nn_dot(a, b):
    return jnp.dot(a, b, preferred_element_type=f32)


def picked_row(rows, at):
    rows = rows.astype(f32)
    return jnp.sum(jnp.where(iota(rows.shape, 0) == at, rows, 0.0), axis=0, keepdims=True)


def prep_kernel(idx_ref, query_ref, far_nope_ref, far_rope_ref, out_ref):
    first = idx_ref[0] % CORES == 0

    def padded(row):
        row = row.astype(f32)
        return jnp.concatenate([row, jnp.zeros((1, LANES - row.shape[1]), f32)], axis=1)

    own = query_ref[0, :1, :NOPE].astype(f32), padded(query_ref[0, :1, NOPE:])
    far = far_nope_ref[0, :1].astype(f32), padded(far_rope_ref[0, :1])
    shape = (out_ref.shape[0], LANES)
    line = iota(shape, 0) % (2 * CORES)
    near = (line < 2) == first
    rows = jnp.where(
        near, jnp.where(line % 2 == 0, own[0], own[1]), jnp.where(line % 2 == 0, far[0], far[1])
    )
    out_ref[...] = rows.astype(bf16)


def by_head(rows):
    wide = jnp.concatenate([rows] * HEADS, axis=1)
    diagonal = iota(wide.shape, 1) // rows.shape[1] == iota(wide.shape, 0)
    return jnp.where(diagonal, wide, jnp.zeros_like(wide))


def slab_request(map_ref, slot):
    owners = map_ref[...]
    place = iota(owners.shape, 1) // SLABS_REQ
    return jnp.sum(jnp.where(owners == slot, place, 0), axis=1, keepdims=True)


def length_of(lengths_ref, req):
    lengths = lengths_ref[...]
    mine = jnp.where(iota(lengths.shape, 1) == req, lengths, 0)
    return jnp.sum(mine, axis=1, keepdims=True)


def attend_kernel(
    idx_ref,
    lengths_ref,
    got_ref,
    w_uk_ref,
    w_uv_ref,
    slab_ref,
    slab_pos_ref,
    map_ref,
    keep_ref,
    give_ref,
    up_ref,
    level_ref,
):
    holder = idx_ref[0]
    core = holder % CORES
    req_v = slab_request(map_ref, holder)

    shape = (2 * HEADS, got_ref.shape[0])
    part = iota(shape, 0)
    want = (req_v * HEADS + part % HEADS) * 2 + part // HEADS
    pick = jnp.where(iota(shape, 1) == want, 1.0, 0.0).astype(bf16)
    q_all = nn_dot(pick, got_ref[...]).astype(bf16)
    rope_dim = slab_ref.shape[2] - LATENT
    q_nope, q_rope = q_all[:HEADS], q_all[HEADS:, :rope_dim]

    q_lat = nn_dot(by_head(q_nope), w_uk_ref[0].reshape(-1, LATENT)).astype(bf16)

    latent = slab_ref[0, 0, :LATENT]
    rotary = slab_ref[0, 0, LATENT:]
    score = (nn_dot(q_lat, latent) + nn_dot(q_rope, rotary)) * score_scale
    live = slab_pos_ref[0] < length_of(lengths_ref, req_v)
    top = jnp.max(jnp.where(live, score, neg_fill), axis=1, keepdims=True)
    weight = jnp.where(live, jnp.exp(jnp.where(live, score - top, 0.0)), 0.0).astype(bf16)
    total = jnp.sum(weight.astype(f32), axis=1, keepdims=True)
    safe = jnp.where(total > 0.0, total, 1.0)
    out = nt_dot(weight, latent) / safe
    level = jnp.where(total > 0.0, top + jnp.log(safe), neg_fill)

    up_ref[...] = nn_dot(by_head(out.astype(bf16)), w_uv_ref[0].reshape(-1, LANES))
    level_ref[...] = jnp.broadcast_to(level, level_ref.shape)
    half = HEADS // CORES
    for ref, first in ((keep_ref, core), (give_ref, 1 - core)):
        ref[:half] = up_ref[pl.ds(first, half, stride=CORES), :]
        ref[half:] = level_ref[pl.ds(first, half, stride=CORES), :]


def own_kernel(
    idx_ref,
    lengths_ref,
    query_ref,
    w_uk_ref,
    w_uv_ref,
    newlat_ref,
    map_ref,
    deep_ref,
    deep_pos_ref,
    aux_ref,
    chips_ref,
):
    holder = idx_ref[0]
    own_req = holder // HEADS
    own_head = holder % HEADS
    nope, rope = query_ref[0, :, :NOPE], query_ref[0, :, NOPE:]

    own_lat = nn_dot(nope[:1], w_uk_ref[0, own_head]).astype(bf16).astype(f32)
    newlat = picked_row(newlat_ref[0], own_req)
    own_score = (
        jnp.sum(own_lat * newlat[:, :LATENT], axis=1, keepdims=True)
        + jnp.sum(rope[:1].astype(f32) * newlat[:, LATENT:], axis=1, keepdims=True)
    ) * score_scale
    aux_ref[0:1, :] = nn_dot(newlat[:, :LATENT].astype(bf16), w_uv_ref[0, own_head])
    aux_ref[1:2, :] = jnp.broadcast_to(own_score, (1, LANES))

    own_lat = nn_dot(nope[1:], w_uk_ref[1, own_head]).astype(bf16)
    latent = deep_ref[0, own_req, :LATENT]
    rotary = deep_ref[0, own_req, LATENT:]
    score = (nn_dot(own_lat, latent) + nn_dot(rope[1:], rotary)) * score_scale
    live = deep_pos_ref[0, pl.ds(own_req, 1), :] < length_of(lengths_ref, own_req)
    block_max = jnp.max(jnp.where(live, score, neg_fill), axis=1, keepdims=True)
    weight = jnp.where(live, jnp.exp(jnp.where(live, score - block_max, 0.0)), 0.0).astype(bf16)
    block_sum = jnp.sum(weight.astype(f32), axis=1, keepdims=True)
    block_out = nt_dot(weight, latent)
    newlat = picked_row(newlat_ref[1], own_req)
    own_score = (
        jnp.sum(own_lat.astype(f32) * newlat[:, :LATENT], axis=1, keepdims=True)
        + jnp.sum(rope[1:].astype(f32) * newlat[:, LATENT:], axis=1, keepdims=True)
    ) * score_scale
    top = jnp.maximum(own_score, block_max)
    own_factor = jnp.exp(own_score - top)
    far_factor = jnp.exp(block_max - top)
    total = own_factor + block_sum * far_factor
    mixed = ((own_factor * newlat[:, :LATENT] + block_out * far_factor) / total).astype(bf16)
    aux_ref[2:3, :] = nn_dot(mixed, w_uv_ref[1, own_head])

    for row, slot in ((3, holder), (4, holder + 1 - 2 * (holder % CORES))):
        req = slab_request(map_ref, slot).astype(f32)
        aux_ref[row : row + 1, :] = jnp.broadcast_to(req, (1, LANES))

    shape = chips_ref.shape
    place = iota(shape, 1) == own_req * SLABS_REQ + iota(shape, 0)
    slots = jnp.sum(jnp.where(place, map_ref[...], 0), axis=1, keepdims=True)
    chips_ref[...] = jnp.broadcast_to(slots // CORES, shape)


def merge_kernel(keep_ref, far_ref, aux_ref, send_ref):
    near_req, far_req = aux_ref[3:4, :], aux_ref[4:5, :]
    half = keep_ref.shape[0] // 2
    near, near_level = keep_ref[:half], keep_ref[half:]
    far, far_level = far_ref[:half], far_ref[half:]
    top = jnp.maximum(near_level, far_level)
    near_factor, far_factor = jnp.exp(near_level - top), jnp.exp(far_level - top)
    total = near_factor + far_factor
    merged = (near_factor * near + far_factor * far) / total
    level = top + (jnp.log(total) - LOG_2)
    same = near_req == far_req
    near, near_level = jnp.where(same, merged, near), jnp.where(same, level, near_level)
    far, far_level = jnp.where(same, merged, far), jnp.where(same, level, far_level)
    for b in range(send_ref.shape[0] // (half * MSG)):
        mine = near_req == b
        first = b * half * MSG
        send_ref[pl.ds(first, half, stride=MSG), :] = jnp.where(mine, near, far)
        send_ref[pl.ds(first + 1, half, stride=MSG), :] = jnp.where(mine, near_level, far_level)


def combine_kernel(chips_ref, got_ref, aux_ref, out_ref):
    chips = chips_ref[...]
    own_score = aux_ref[1:2, :]
    values, levels = [aux_ref[0:1, :]], [own_score]
    for s in range(SLABS_REQ):
        row = chips[s, 0] * MSG
        values.append(got_ref[pl.ds(row, 1), :])
        levels.append(got_ref[pl.ds(row + 1, 1), :])
    values, levels = jnp.concatenate(values, axis=0), jnp.concatenate(levels, axis=0)
    factors = jnp.exp(levels - jnp.max(levels, axis=0, keepdims=True))
    total = jnp.sum(factors, axis=0, keepdims=True)
    attended = jnp.sum(factors * values, axis=0, keepdims=True) / total
    out_ref[0] = jnp.concatenate([attended, aux_ref[2:3, :]], axis=0).astype(bf16)


VMEM = pl.BlockSpec(memory_space=pltpu.VMEM)
SMEM = pl.BlockSpec(memory_space=pltpu.SMEM)


def call(kernel, out_shape, in_specs, flops, scratch_shapes=()):
    many = isinstance(out_shape, tuple)
    return pl.pallas_call(
        kernel,
        out_shape=out_shape,
        in_specs=in_specs,
        out_specs=(VMEM,) * len(out_shape) if many else VMEM,
        scratch_shapes=scratch_shapes,
        compiler_params=pltpu.CompilerParams(vmem_limit_bytes=12 << 20),
        cost_estimate=pl.CostEstimate(flops=flops, bytes_accessed=1 << 20, transcendentals=0),
    )


def exchanged(rows, per_chip):
    chips = lax.axis_size("chips")
    tiles = rows.reshape(chips, per_chip, LANES)
    return lax.all_to_all(tiles, "chips", 0, 0, tiled=True).reshape(rows.shape)


def swapped(x):
    return lax.ppermute(x, "cores", [(k, (k + 1) % CORES) for k in range(CORES)])


def shards(
    q_nope,
    q_rope,
    w_uk,
    w_uv,
    new_latent,
    shallow_cache,
    slot_positions,
    slab_map,
    deep_cache,
    deep_positions,
    lengths,
):
    chips = lax.axis_size("chips")
    holder = lax.axis_index("chips") * CORES + lax.axis_index("cores")
    holder = holder.astype(jnp.int32).reshape(1)
    shape = jax.ShapeDtypeStruct
    q_nope, q_rope = q_nope.swapaxes(0, 1), q_rope.swapaxes(0, 1)
    shallow_cache, deep_cache = shallow_cache.swapaxes(2, 3), deep_cache.swapaxes(2, 3)
    far_nope, far_rope = swapped(q_nope), swapped(q_rope)
    query = jnp.concatenate([q_nope, q_rope], axis=-1)
    queries = call(
        prep_kernel, shape((chips * CORES * 2, LANES), bf16), [SMEM] + [VMEM] * 3, 1 << 33
    )(holder, query, far_nope, far_rope)
    queries = exchanged(queries, CORES * 2)
    block = shape((HEADS // CORES * MSG, LANES), f32)
    lengths = lengths.reshape(1, -1)
    keep, give = call(
        attend_kernel,
        (block, block),
        [SMEM] + [VMEM] * 7,
        1 << 24,
        [pltpu.VMEM((HEADS, LANES), f32)] * 2,
    )(holder, lengths, queries, w_uk, w_uv, shallow_cache, slot_positions, slab_map)
    far = swapped(give)
    aux, slab_chips = call(
        own_kernel,
        (shape((8, LANES), f32), shape((SLABS_REQ, LANES), jnp.int32)),
        [SMEM] + [VMEM] * 8,
        1 << 24,
    )(
        holder, lengths, query, w_uk, w_uv, new_latent, slab_map, deep_cache, deep_positions
    )
    partials = call(merge_kernel, shape((chips * MSG, LANES), f32), [VMEM] * 3, 1 << 20)(
        keep, far, aux
    )
    partials = exchanged(partials, MSG)
    rows = call(combine_kernel, shape(q_nope.shape, bf16), [VMEM] * 3, 1 << 20)(
        slab_chips, partials, aux
    )
    return rows.swapaxes(0, 1)


def solution(mesh):
    groups, holders = mesh.shape["groups"], mesh.shape["holders"]
    mesh = Mesh(
        mesh.devices.reshape(groups, holders // CORES, CORES), ("groups", "chips", "cores")
    )
    spread = ("groups", "chips", "cores")
    in_specs = (
        P(None, spread, None),
        P(None, spread, None),
        P(),
        P(),
        P(None, "groups", None),
        P(None, spread, None, None),
        P(None, spread, None),
        P(None, "groups"),
        P(None, "groups", None, None),
        P(None, "groups", None),
        P("groups"),
    )
    return jax.shard_map(
        shards, mesh=mesh, in_specs=in_specs, out_specs=P(None, spread, None), check_vma=False
    )
```

```python
import math

import jax
import jax.numpy as jnp
from jax import lax
from jax.experimental import pallas as pl
from jax.experimental.pallas import tpu as pltpu
from jax.sharding import Mesh
from jax.sharding import PartitionSpec as P

HEADS = 16
LATENT = 512
NOPE = 128
SLABS_REQ = 16
LANES = 128
MSG = 2
CORES = 2
LOG_2 = math.log(2.0)

score_scale = 192.0 ** (-0.5)
neg_fill = -1e30
f32 = jnp.float32
bf16 = jnp.bfloat16


def iota(shape, dim):
    return lax.broadcasted_iota(jnp.int32, shape, dim)


def nt_dot(a, b):
    return lax.dot_general(a, b, (((1,), (1,)), ((), ())), preferred_element_type=f32)


def nn_dot(a, b):
    return jnp.dot(a, b, preferred_element_type=f32)


def picked_row(rows, at):
    rows = rows.astype(f32)
    return jnp.sum(jnp.where(iota(rows.shape, 0) == at, rows, 0.0), axis=0, keepdims=True)


def prep_kernel(idx_ref, query_ref, far_nope_ref, far_rope_ref, out_ref):
    first = idx_ref[0] % CORES == 0

    def padded(row):
        row = row.astype(f32)
        return jnp.concatenate([row, jnp.zeros((1, LANES - row.shape[1]), f32)], axis=1)

    own = query_ref[0, :1, :NOPE].astype(f32), padded(query_ref[0, :1, NOPE:])
    far = far_nope_ref[0, :1].astype(f32), padded(far_rope_ref[0, :1])
    shape = (out_ref.shape[0], LANES)
    line = iota(shape, 0) % (2 * CORES)
    near = (line < 2) == first
    rows = jnp.where(
        near, jnp.where(line % 2 == 0, own[0], own[1]), jnp.where(line % 2 == 0, far[0], far[1])
    )
    out_ref[...] = rows.astype(bf16)


def by_head(rows):
    wide = jnp.concatenate([rows] * rows.shape[0], axis=1)
    diagonal = iota(wide.shape, 1) // rows.shape[1] == iota(wide.shape, 0)
    return jnp.where(diagonal, wide, jnp.zeros_like(wide))


def up_projected(out, w_uv_ref, parity):
    half = HEADS // CORES
    wide = jnp.concatenate([out] * half, axis=1)
    row = iota(wide.shape, 0)
    place = (iota(wide.shape, 1) // LATENT == row // CORES) & (row % CORES == parity)
    heads = [w_uv_ref[0, k * CORES + parity] for k in range(half)]
    return nn_dot(
        jnp.where(place, wide, jnp.zeros_like(wide)), jnp.concatenate(heads, axis=0)
    )


def slab_request(map_ref, slot):
    owners = map_ref[...]
    place = iota(owners.shape, 1) // SLABS_REQ
    return jnp.sum(jnp.where(owners == slot, place, 0), axis=1, keepdims=True)


def length_of(lengths_ref, req):
    lengths = lengths_ref[...]
    mine = jnp.where(iota(lengths.shape, 1) == req, lengths, 0)
    return jnp.sum(mine, axis=1, keepdims=True)


def attend_kernel(
    idx_ref,
    lengths_ref,
    got_ref,
    w_uk_ref,
    w_uv_ref,
    slab_ref,
    slab_pos_ref,
    map_ref,
    keep_ref,
    give_ref,
    level_ref,
    rows_ref,
    all_level_ref,
):
    holder = idx_ref[0]
    core = holder % CORES
    req_v = slab_request(map_ref, holder)

    shape = (2 * HEADS, got_ref.shape[0])
    part = iota(shape, 0)
    want = (req_v * HEADS + part % HEADS) * 2 + part // HEADS
    pick = jnp.where(iota(shape, 1) == want, 1.0, 0.0).astype(bf16)
    q_all = nn_dot(pick, got_ref[...]).astype(bf16)
    rope_dim = slab_ref.shape[2] - LATENT
    q_nope, q_rope = q_all[:HEADS], q_all[HEADS:, :rope_dim]

    q_lat = nn_dot(by_head(q_nope), w_uk_ref[0].reshape(-1, LATENT)).astype(bf16)

    latent = slab_ref[0, 0, :LATENT]
    rotary = slab_ref[0, 0, LATENT:]
    score = (nn_dot(q_lat, latent) + nn_dot(q_rope, rotary)) * score_scale
    live = slab_pos_ref[0] < length_of(lengths_ref, req_v)
    top = jnp.max(jnp.where(live, score, neg_fill), axis=1, keepdims=True)
    weight = jnp.where(live, jnp.exp(jnp.where(live, score - top, 0.0)), 0.0).astype(bf16)
    total = jnp.sum(weight.astype(f32), axis=1, keepdims=True)
    safe = jnp.where(total > 0.0, total, 1.0)
    out = nt_dot(weight, latent) / safe
    level = jnp.where(total > 0.0, top + jnp.log(safe), neg_fill)

    out = out.astype(bf16)
    keep_ref[...] = out
    rows_ref[...] = up_projected(out, w_uv_ref, 1 - core)
    all_level_ref[...] = jnp.broadcast_to(level, all_level_ref.shape)
    half = HEADS // CORES
    give_ref[:half] = rows_ref[pl.ds(1 - core, half, stride=CORES), :]
    give_ref[half:] = all_level_ref[pl.ds(1 - core, half, stride=CORES), :]
    level_ref[...] = all_level_ref[pl.ds(core, half, stride=CORES), :]


def own_kernel(
    idx_ref,
    lengths_ref,
    query_ref,
    w_uk_ref,
    w_uv_ref,
    newlat_ref,
    map_ref,
    deep_ref,
    deep_pos_ref,
    keep_ref,
    aux_ref,
    chips_ref,
    up_ref,
    rows_ref,
):
    holder = idx_ref[0]
    own_req = holder // HEADS
    own_head = holder % HEADS
    nope, rope = query_ref[0, :, :NOPE], query_ref[0, :, NOPE:]

    own_lat = nn_dot(nope[:1], w_uk_ref[0, own_head]).astype(bf16).astype(f32)
    newlat = picked_row(newlat_ref[0], own_req)
    own_score = (
        jnp.sum(own_lat * newlat[:, :LATENT], axis=1, keepdims=True)
        + jnp.sum(rope[:1].astype(f32) * newlat[:, LATENT:], axis=1, keepdims=True)
    ) * score_scale
    aux_ref[0:1, :] = nn_dot(newlat[:, :LATENT].astype(bf16), w_uv_ref[0, own_head])
    aux_ref[1:2, :] = jnp.broadcast_to(own_score, (1, LANES))

    own_lat = nn_dot(nope[1:], w_uk_ref[1, own_head]).astype(bf16)
    latent = deep_ref[0, own_req, :LATENT]
    rotary = deep_ref[0, own_req, LATENT:]
    score = (nn_dot(own_lat, latent) + nn_dot(rope[1:], rotary)) * score_scale
    live = deep_pos_ref[0, pl.ds(own_req, 1), :] < length_of(lengths_ref, own_req)
    block_max = jnp.max(jnp.where(live, score, neg_fill), axis=1, keepdims=True)
    weight = jnp.where(live, jnp.exp(jnp.where(live, score - block_max, 0.0)), 0.0).astype(bf16)
    block_sum = jnp.sum(weight.astype(f32), axis=1, keepdims=True)
    block_out = nt_dot(weight, latent)
    newlat = picked_row(newlat_ref[1], own_req)
    own_score = (
        jnp.sum(own_lat.astype(f32) * newlat[:, :LATENT], axis=1, keepdims=True)
        + jnp.sum(rope[1:].astype(f32) * newlat[:, LATENT:], axis=1, keepdims=True)
    ) * score_scale
    top = jnp.maximum(own_score, block_max)
    own_factor = jnp.exp(own_score - top)
    far_factor = jnp.exp(block_max - top)
    total = own_factor + block_sum * far_factor
    mixed = ((own_factor * newlat[:, :LATENT] + block_out * far_factor) / total).astype(bf16)
    aux_ref[2:3, :] = nn_dot(mixed, w_uv_ref[1, own_head])

    for row, slot in ((3, holder), (4, holder + 1 - 2 * (holder % CORES))):
        req = slab_request(map_ref, slot).astype(f32)
        aux_ref[row : row + 1, :] = jnp.broadcast_to(req, (1, LANES))

    core = holder % CORES
    rows_ref[...] = up_projected(keep_ref[...], w_uv_ref, core)
    up_ref[...] = rows_ref[pl.ds(core, HEADS // CORES, stride=CORES), :]

    shape = chips_ref.shape
    place = iota(shape, 1) == own_req * SLABS_REQ + iota(shape, 0)
    slots = jnp.sum(jnp.where(place, map_ref[...], 0), axis=1, keepdims=True)
    chips_ref[...] = jnp.broadcast_to(slots // CORES, shape)


def merge_kernel(near_ref, near_level_ref, far_ref, aux_ref, send_ref):
    near_req, far_req = aux_ref[3:4, :], aux_ref[4:5, :]
    half = near_ref.shape[0]
    near, near_level = near_ref[...], near_level_ref[...]
    far, far_level = far_ref[:half], far_ref[half:]
    top = jnp.maximum(near_level, far_level)
    near_factor, far_factor = jnp.exp(near_level - top), jnp.exp(far_level - top)
    total = near_factor + far_factor
    merged = (near_factor * near + far_factor * far) / total
    level = top + (jnp.log(total) - LOG_2)
    same = near_req == far_req
    near, near_level = jnp.where(same, merged, near), jnp.where(same, level, near_level)
    far, far_level = jnp.where(same, merged, far), jnp.where(same, level, far_level)
    for b in range(send_ref.shape[0] // (half * MSG)):
        mine = near_req == b
        first = b * half * MSG
        send_ref[pl.ds(first, half, stride=MSG), :] = jnp.where(mine, near, far)
        send_ref[pl.ds(first + 1, half, stride=MSG), :] = jnp.where(mine, near_level, far_level)


def combine_kernel(chips_ref, got_ref, aux_ref, out_ref):
    chips = chips_ref[...]
    own_score = aux_ref[1:2, :]
    values, levels = [aux_ref[0:1, :]], [own_score]
    for s in range(SLABS_REQ):
        row = chips[s, 0] * MSG
        values.append(got_ref[pl.ds(row, 1), :])
        levels.append(got_ref[pl.ds(row + 1, 1), :])
    values, levels = jnp.concatenate(values, axis=0), jnp.concatenate(levels, axis=0)
    factors = jnp.exp(levels - jnp.max(levels, axis=0, keepdims=True))
    total = jnp.sum(factors, axis=0, keepdims=True)
    attended = jnp.sum(factors * values, axis=0, keepdims=True) / total
    out_ref[0] = jnp.concatenate([attended, aux_ref[2:3, :]], axis=0).astype(bf16)


VMEM = pl.BlockSpec(memory_space=pltpu.VMEM)
SMEM = pl.BlockSpec(memory_space=pltpu.SMEM)


def call(kernel, out_shape, in_specs, flops, scratch_shapes=()):
    many = isinstance(out_shape, tuple)
    return pl.pallas_call(
        kernel,
        out_shape=out_shape,
        in_specs=in_specs,
        out_specs=(VMEM,) * len(out_shape) if many else VMEM,
        scratch_shapes=scratch_shapes,
        compiler_params=pltpu.CompilerParams(vmem_limit_bytes=12 << 20),
        cost_estimate=pl.CostEstimate(flops=flops, bytes_accessed=1 << 20, transcendentals=0),
    )


def exchanged(rows, per_chip):
    chips = lax.axis_size("chips")
    tiles = rows.reshape(chips, per_chip, LANES)
    return lax.all_to_all(tiles, "chips", 0, 0, tiled=True).reshape(rows.shape)


def swapped(x):
    return lax.ppermute(x, "cores", [(k, (k + 1) % CORES) for k in range(CORES)])


def shards(
    q_nope,
    q_rope,
    w_uk,
    w_uv,
    new_latent,
    shallow_cache,
    slot_positions,
    slab_map,
    deep_cache,
    deep_positions,
    lengths,
):
    chips = lax.axis_size("chips")
    holder = lax.axis_index("chips") * CORES + lax.axis_index("cores")
    holder = holder.astype(jnp.int32).reshape(1)
    shape = jax.ShapeDtypeStruct
    q_nope, q_rope = q_nope.swapaxes(0, 1), q_rope.swapaxes(0, 1)
    shallow_cache, deep_cache = shallow_cache.swapaxes(2, 3), deep_cache.swapaxes(2, 3)
    far_nope, far_rope = swapped(q_nope), swapped(q_rope)
    query = jnp.concatenate([q_nope, q_rope], axis=-1)
    queries = call(
        prep_kernel, shape((chips * CORES * 2, LANES), bf16), [SMEM] + [VMEM] * 3, 1 << 33
    )(holder, query, far_nope, far_rope)
    queries = exchanged(queries, CORES * 2)
    half = HEADS // CORES
    lengths = lengths.reshape(1, -1)
    keep, give, level = call(
        attend_kernel,
        (
            shape((HEADS, LATENT), bf16),
            shape((half * MSG, LANES), f32),
            shape((half, LANES), f32),
        ),
        [SMEM] + [VMEM] * 7,
        1 << 24,
        [pltpu.VMEM((HEADS, LANES), f32)] * 2,
    )(holder, lengths, queries, w_uk, w_uv, shallow_cache, slot_positions, slab_map)
    far = swapped(give)
    aux, slab_chips, near = call(
        own_kernel,
        (
            shape((8, LANES), f32),
            shape((SLABS_REQ, LANES), jnp.int32),
            shape((half, LANES), f32),
        ),
        [SMEM] + [VMEM] * 9,
        1 << 24,
        [pltpu.VMEM((HEADS, LANES), f32)],
    )(
        holder, lengths, query, w_uk, w_uv, new_latent, slab_map, deep_cache, deep_positions, keep
    )
    partials = call(merge_kernel, shape((chips * MSG, LANES), f32), [VMEM] * 4, 1 << 20)(
        near, level, far, aux
    )
    partials = exchanged(partials, MSG)
    rows = call(combine_kernel, shape(q_nope.shape, bf16), [VMEM] * 3, 1 << 20)(
        slab_chips, partials, aux
    )
    return rows.swapaxes(0, 1)


def solution(mesh):
    groups, holders = mesh.shape["groups"], mesh.shape["holders"]
    mesh = Mesh(
        mesh.devices.reshape(groups, holders // CORES, CORES), ("groups", "chips", "cores")
    )
    spread = ("groups", "chips", "cores")
    in_specs = (
        P(None, spread, None),
        P(None, spread, None),
        P(),
        P(),
        P(None, "groups", None),
        P(None, spread, None, None),
        P(None, spread, None),
        P(None, "groups"),
        P(None, "groups", None, None),
        P(None, "groups", None),
        P("groups"),
    )
    return jax.shard_map(
        shards, mesh=mesh, in_specs=in_specs, out_specs=P(None, spread, None), check_vma=False
    )
```

```python
import math

import jax
import jax.numpy as jnp
from jax import lax
from jax.experimental import pallas as pl
from jax.experimental.pallas import tpu as pltpu
from jax.sharding import Mesh
from jax.sharding import PartitionSpec as P

HEADS = 16
LATENT = 512
NOPE = 128
SLABS_REQ = 16
LANES = 128
MSG = 2
CORES = 2
LOG_2 = math.log(2.0)

score_scale = 192.0 ** (-0.5)
neg_fill = -1e30
f32 = jnp.float32
bf16 = jnp.bfloat16


def iota(shape, dim):
    return lax.broadcasted_iota(jnp.int32, shape, dim)


def nt_dot(a, b):
    return lax.dot_general(a, b, (((1,), (1,)), ((), ())), preferred_element_type=f32)


def nn_dot(a, b):
    return jnp.dot(a, b, preferred_element_type=f32)


def picked_row(rows, at):
    rows = rows.astype(f32)
    return jnp.sum(jnp.where(iota(rows.shape, 0) == at, rows, 0.0), axis=0, keepdims=True)


def prep_kernel(idx_ref, query_ref, far_nope_ref, far_rope_ref, out_ref):
    first = idx_ref[0] % CORES == 0

    def padded(row):
        row = row.astype(f32)
        return jnp.concatenate([row, jnp.zeros((1, LANES - row.shape[1]), f32)], axis=1)

    own = query_ref[0, :1, :NOPE].astype(f32), padded(query_ref[0, :1, NOPE:])
    far = far_nope_ref[0, :1].astype(f32), padded(far_rope_ref[0, :1])
    shape = (out_ref.shape[0], LANES)
    line = iota(shape, 0) % (2 * CORES)
    near = (line < 2) == first
    rows = jnp.where(
        near, jnp.where(line % 2 == 0, own[0], own[1]), jnp.where(line % 2 == 0, far[0], far[1])
    )
    out_ref[...] = rows.astype(bf16)


def by_head(rows):
    wide = jnp.concatenate([rows] * rows.shape[0], axis=1)
    diagonal = iota(wide.shape, 1) // rows.shape[1] == iota(wide.shape, 0)
    return jnp.where(diagonal, wide, jnp.zeros_like(wide))


def up_projected(out, w_uv_ref, parity):
    half = HEADS // CORES
    wide = jnp.concatenate([out] * half, axis=1)
    row = iota(wide.shape, 0)
    place = (iota(wide.shape, 1) // LATENT == row // CORES) & (row % CORES == parity)
    heads = [w_uv_ref[0, k * CORES + parity] for k in range(half)]
    return nn_dot(
        jnp.where(place, wide, jnp.zeros_like(wide)), jnp.concatenate(heads, axis=0)
    )


def slab_request(map_ref, slot):
    owners = map_ref[...]
    place = iota(owners.shape, 1) // SLABS_REQ
    return jnp.sum(jnp.where(owners == slot, place, 0), axis=1, keepdims=True)


def length_of(lengths_ref, req):
    lengths = lengths_ref[...]
    mine = jnp.where(iota(lengths.shape, 1) == req, lengths, 0)
    return jnp.sum(mine, axis=1, keepdims=True)


def attend_kernel(
    idx_ref,
    lengths_ref,
    got_ref,
    w_uk_ref,
    w_uv_ref,
    slab_ref,
    slab_pos_ref,
    map_ref,
    keep_ref,
    give_ref,
    level_ref,
    rows_ref,
    all_level_ref,
):
    holder = idx_ref[0]
    core = holder % CORES
    req_v = slab_request(map_ref, holder)

    shape = (2 * HEADS, got_ref.shape[0])
    part = iota(shape, 0)
    want = (req_v * HEADS + part % HEADS) * 2 + part // HEADS
    pick = jnp.where(iota(shape, 1) == want, 1.0, 0.0).astype(bf16)
    q_all = nn_dot(pick, got_ref[...]).astype(bf16)
    rope_dim = slab_ref.shape[2] - LATENT
    q_nope, q_rope = q_all[:HEADS], q_all[HEADS:, :rope_dim]

    q_lat = nn_dot(by_head(q_nope), w_uk_ref[0].reshape(-1, LATENT)).astype(bf16)

    latent = slab_ref[0, 0, :LATENT]
    rotary = slab_ref[0, 0, LATENT:]
    score = (nn_dot(q_lat, latent) + nn_dot(q_rope, rotary)) * score_scale
    live = slab_pos_ref[0] < length_of(lengths_ref, req_v)
    score = jnp.where(live, score, neg_fill)
    top = jnp.max(score, axis=1, keepdims=True)
    weight = jnp.where(live, jnp.exp(score - top), 0.0).astype(bf16)
    total = jnp.sum(weight.astype(f32), axis=1, keepdims=True)
    safe = jnp.where(total > 0.0, total, 1.0)
    out = nt_dot(weight, latent) / safe
    level = jnp.where(total > 0.0, top + jnp.log(safe), neg_fill)

    out = out.astype(bf16)
    keep_ref[...] = out
    rows_ref[...] = up_projected(out, w_uv_ref, 1 - core)
    all_level_ref[...] = jnp.broadcast_to(level, all_level_ref.shape)
    half = HEADS // CORES
    give_ref[:half] = rows_ref[pl.ds(1 - core, half, stride=CORES), :]
    give_ref[half:] = all_level_ref[pl.ds(1 - core, half, stride=CORES), :]
    level_ref[...] = all_level_ref[pl.ds(core, half, stride=CORES), :]


def own_kernel(
    idx_ref,
    lengths_ref,
    query_ref,
    w_uk_ref,
    w_uv_ref,
    newlat_ref,
    map_ref,
    deep_ref,
    deep_pos_ref,
    keep_ref,
    aux_ref,
    chips_ref,
    up_ref,
    rows_ref,
):
    holder = idx_ref[0]
    own_req = holder // HEADS
    own_head = holder % HEADS
    nope, rope = query_ref[0, :, :NOPE], query_ref[0, :, NOPE:]

    own_lat = nn_dot(nope[:1], w_uk_ref[0, own_head]).astype(bf16).astype(f32)
    newlat = picked_row(newlat_ref[0], own_req)
    own_score = (
        jnp.sum(own_lat * newlat[:, :LATENT], axis=1, keepdims=True)
        + jnp.sum(rope[:1].astype(f32) * newlat[:, LATENT:], axis=1, keepdims=True)
    ) * score_scale
    aux_ref[0:1, :] = nn_dot(newlat[:, :LATENT].astype(bf16), w_uv_ref[0, own_head])
    aux_ref[1:2, :] = jnp.broadcast_to(own_score, (1, LANES))

    own_lat = nn_dot(nope[1:], w_uk_ref[1, own_head]).astype(bf16)
    latent = deep_ref[0, own_req, :LATENT]
    rotary = deep_ref[0, own_req, LATENT:]
    score = (nn_dot(own_lat, latent) + nn_dot(rope[1:], rotary)) * score_scale
    live = deep_pos_ref[0, pl.ds(own_req, 1), :] < length_of(lengths_ref, own_req)
    score = jnp.where(live, score, neg_fill)
    block_max = jnp.max(score, axis=1, keepdims=True)
    weight = jnp.where(live, jnp.exp(score - block_max), 0.0).astype(bf16)
    block_sum = jnp.sum(weight.astype(f32), axis=1, keepdims=True)
    block_out = nt_dot(weight, latent)
    newlat = picked_row(newlat_ref[1], own_req)
    own_score = (
        jnp.sum(own_lat.astype(f32) * newlat[:, :LATENT], axis=1, keepdims=True)
        + jnp.sum(rope[1:].astype(f32) * newlat[:, LATENT:], axis=1, keepdims=True)
    ) * score_scale
    top = jnp.maximum(own_score, block_max)
    own_factor = jnp.exp(own_score - top)
    far_factor = jnp.exp(block_max - top)
    total = own_factor + block_sum * far_factor
    mixed = ((own_factor * newlat[:, :LATENT] + block_out * far_factor) / total).astype(bf16)
    aux_ref[2:3, :] = nn_dot(mixed, w_uv_ref[1, own_head])

    for row, slot in ((3, holder), (4, holder + 1 - 2 * (holder % CORES))):
        req = slab_request(map_ref, slot).astype(f32)
        aux_ref[row : row + 1, :] = jnp.broadcast_to(req, (1, LANES))

    core = holder % CORES
    rows_ref[...] = up_projected(keep_ref[...], w_uv_ref, core)
    up_ref[...] = rows_ref[pl.ds(core, HEADS // CORES, stride=CORES), :]

    shape = chips_ref.shape
    place = iota(shape, 1) == own_req * SLABS_REQ + iota(shape, 0)
    slots = jnp.sum(jnp.where(place, map_ref[...], 0), axis=1, keepdims=True)
    chips_ref[...] = jnp.broadcast_to(slots // CORES, shape)


def merge_kernel(near_ref, near_level_ref, far_ref, aux_ref, send_ref):
    near_req, far_req = aux_ref[3:4, :], aux_ref[4:5, :]
    half = near_ref.shape[0]
    near, near_level = near_ref[...], near_level_ref[...]
    far, far_level = far_ref[:half], far_ref[half:]
    top = jnp.maximum(near_level, far_level)
    near_factor, far_factor = jnp.exp(near_level - top), jnp.exp(far_level - top)
    total = near_factor + far_factor
    merged = (near_factor * near + far_factor * far) / total
    level = top + (jnp.log(total) - LOG_2)
    same = near_req == far_req
    near, near_level = jnp.where(same, merged, near), jnp.where(same, level, near_level)
    far, far_level = jnp.where(same, merged, far), jnp.where(same, level, far_level)
    for b in range(send_ref.shape[0] // (half * MSG)):
        mine = near_req == b
        first = b * half * MSG
        send_ref[pl.ds(first, half, stride=MSG), :] = jnp.where(mine, near, far)
        send_ref[pl.ds(first + 1, half, stride=MSG), :] = jnp.where(mine, near_level, far_level)


def combine_kernel(chips_ref, got_ref, aux_ref, out_ref):
    chips = chips_ref[...]
    own_score = aux_ref[1:2, :]
    values, levels = [aux_ref[0:1, :]], [own_score]
    for s in range(SLABS_REQ):
        row = chips[s, 0] * MSG
        values.append(got_ref[pl.ds(row, 1), :])
        levels.append(got_ref[pl.ds(row + 1, 1), :])
    values, levels = jnp.concatenate(values, axis=0), jnp.concatenate(levels, axis=0)
    factors = jnp.exp(levels - jnp.max(levels, axis=0, keepdims=True))
    total = jnp.sum(factors, axis=0, keepdims=True)
    attended = jnp.sum(factors * values, axis=0, keepdims=True) / total
    out_ref[0] = jnp.concatenate([attended, aux_ref[2:3, :]], axis=0).astype(bf16)


VMEM = pl.BlockSpec(memory_space=pltpu.VMEM)
SMEM = pl.BlockSpec(memory_space=pltpu.SMEM)


def call(kernel, out_shape, in_specs, flops, scratch_shapes=()):
    many = isinstance(out_shape, tuple)
    return pl.pallas_call(
        kernel,
        out_shape=out_shape,
        in_specs=in_specs,
        out_specs=(VMEM,) * len(out_shape) if many else VMEM,
        scratch_shapes=scratch_shapes,
        compiler_params=pltpu.CompilerParams(vmem_limit_bytes=12 << 20),
        cost_estimate=pl.CostEstimate(flops=flops, bytes_accessed=1 << 20, transcendentals=0),
    )


def exchanged(rows, per_chip):
    chips = lax.axis_size("chips")
    tiles = rows.reshape(chips, per_chip, LANES)
    return lax.all_to_all(tiles, "chips", 0, 0, tiled=True).reshape(rows.shape)


def swapped(x):
    return lax.ppermute(x, "cores", [(k, (k + 1) % CORES) for k in range(CORES)])


def shards(
    q_nope,
    q_rope,
    w_uk,
    w_uv,
    new_latent,
    shallow_cache,
    slot_positions,
    slab_map,
    deep_cache,
    deep_positions,
    lengths,
):
    chips = lax.axis_size("chips")
    holder = lax.axis_index("chips") * CORES + lax.axis_index("cores")
    holder = holder.astype(jnp.int32).reshape(1)
    shape = jax.ShapeDtypeStruct
    q_nope, q_rope = q_nope.swapaxes(0, 1), q_rope.swapaxes(0, 1)
    shallow_cache, deep_cache = shallow_cache.swapaxes(2, 3), deep_cache.swapaxes(2, 3)
    far_nope, far_rope = swapped(q_nope), swapped(q_rope)
    query = jnp.concatenate([q_nope, q_rope], axis=-1)
    queries = call(
        prep_kernel, shape((chips * CORES * 2, LANES), bf16), [SMEM] + [VMEM] * 3, 1 << 33
    )(holder, query, far_nope, far_rope)
    queries = exchanged(queries, CORES * 2)
    half = HEADS // CORES
    lengths = lengths.reshape(1, -1)
    keep, give, level = call(
        attend_kernel,
        (
            shape((HEADS, LATENT), bf16),
            shape((half * MSG, LANES), f32),
            shape((half, LANES), f32),
        ),
        [SMEM] + [VMEM] * 7,
        1 << 24,
        [pltpu.VMEM((HEADS, LANES), f32)] * 2,
    )(holder, lengths, queries, w_uk, w_uv, shallow_cache, slot_positions, slab_map)
    far = swapped(give)
    aux, slab_chips, near = call(
        own_kernel,
        (
            shape((8, LANES), f32),
            shape((SLABS_REQ, LANES), jnp.int32),
            shape((half, LANES), f32),
        ),
        [SMEM] + [VMEM] * 9,
        1 << 24,
        [pltpu.VMEM((HEADS, LANES), f32)],
    )(
        holder, lengths, query, w_uk, w_uv, new_latent, slab_map, deep_cache, deep_positions, keep
    )
    partials = call(merge_kernel, shape((chips * MSG, LANES), f32), [VMEM] * 4, 1 << 20)(
        near, level, far, aux
    )
    partials = exchanged(partials, MSG)
    rows = call(combine_kernel, shape(q_nope.shape, bf16), [VMEM] * 3, 1 << 20)(
        slab_chips, partials, aux
    )
    return rows.swapaxes(0, 1)


def solution(mesh):
    groups, holders = mesh.shape["groups"], mesh.shape["holders"]
    mesh = Mesh(
        mesh.devices.reshape(groups, holders // CORES, CORES), ("groups", "chips", "cores")
    )
    spread = ("groups", "chips", "cores")
    in_specs = (
        P(None, spread, None),
        P(None, spread, None),
        P(),
        P(),
        P(None, "groups", None),
        P(None, spread, None, None),
        P(None, spread, None),
        P(None, "groups"),
        P(None, "groups", None, None),
        P(None, "groups", None),
        P("groups"),
    )
    return jax.shard_map(
        shards, mesh=mesh, in_specs=in_specs, out_specs=P(None, spread, None), check_vma=False
    )
```
